512 devices in a mesh: group: 16 (over z, core), dev: 32 (over x, y).
Axes of the slice: x: 4, y: 8, z: 8, core: 2. Of those that a mesh axis runs over, the one named last changes fastest.
Arguments:
- acts: bfloat16 [196608, 768], P(('group', 'dev')), may hold values from -6 to 6
- grad_out: bfloat16 [196608, 2048], P(('group', 'dev')), may hold values from -0.25 to 0.25
- live_rows: int32 [512], P(('group', 'dev')), may hold values from 96 to 384, as said below
- placement: int32 [512], replicated, may hold values from 0 to 31, as said below
- master: float32 [32, 768, 2048], P('group', 'dev'), may hold values from -0.21875 to 0.21875
- moment1: float32 [32, 768, 2048], P('group', 'dev'), may hold values from -3 to 3
- moment2: float32 [32, 768, 2048], P('group', 'dev'), may hold values from 0.05 to 5
Outputs:
- grad_in: bfloat16 [196608, 768], P(('group', 'dev'))
- new_master: float32 [32, 768, 2048], P('group', 'dev')
- new_moment1: float32 [32, 768, 2048], P('group', 'dev')
- new_moment2: float32 [32, 768, 2048], P('group', 'dev')
The draws below stay inside these ranges and needn't reach their ends.
Inputs may be any that keep to these rules, and one draw needn't show every extreme that they name: `placement`: every expert is named by some device. In each copy group (devices g * 32 to g * 32 + 31), for every index o of group exactly 2 devices run an expert e with e // 2 = o, and they all run the same one. `live_rows`: some device has all 384 slots live.
All inputs are finite; a program needn't handle non-finite values.
Results may differ from the reference program's by a relative error of at most 0.0085.
Values may be sent and summed in bfloat16 or wider, within the bound.
A program may use at most 64 MiB of HBM per device.

```python
import math
import jax
import jax.numpy as jnp
from jax import lax

D = 2048
FF = 768
EXP_GROUP = 2
ROWS = 384
EXPERTS = 32
TOTAL_ROWS = 196608
N_GROUP = 16
N_DEV = 32
DEVICES = 512


def draw_placement(key, part):
    subkeys = jax.random.split(jax.random.fold_in(key, 11), 3)
    heavy = jax.random.randint(subkeys[0], (N_GROUP,), 1, N_GROUP)
    owner_keys = jax.random.split(subkeys[1], N_GROUP)
    orders = jax.vmap(lambda k: jax.random.permutation(k, N_GROUP))(owner_keys)
    picks = (orders < heavy[:, None]).astype(jnp.int32)
    group_keys = jax.random.split(subkeys[2], N_GROUP)
    slots = jax.vmap(lambda k: jax.random.permutation(k, N_DEV))(group_keys)
    owners = (slots % N_GROUP).astype(jnp.int32)
    chosen = picks.T
    bits = jnp.take_along_axis(chosen, owners, axis=1)
    experts = EXP_GROUP * owners + bits
    return experts.reshape(DEVICES).astype(jnp.int32)


def draw_live_rows(key, part):
    subkeys = jax.random.split(jax.random.fold_in(key, 23), 2)
    counts = jax.random.randint(subkeys[0], (DEVICES,), ROWS // 4, ROWS + 1)
    fullest = jax.random.randint(subkeys[1], (), 0, DEVICES)
    return counts.at[fullest].set(ROWS).astype(jnp.int32)


def steps_of(key, extent, shards, smallest, top_value):
    loudness, own = 1.0, jax.random.fold_in(key, 6)
    for axis_at, parts in shards:
        heights = jnp.exp(jax.random.uniform(jax.random.fold_in(own, axis_at), (parts,), jnp.float32, smallest / len(shards), top_value / len(shards)))
        loudness = loudness * jnp.repeat(heights, extent[axis_at] // parts).reshape([-1 if axis == axis_at else 1 for axis in range(len(extent))])
    return loudness


def centred(rng, extent, scale, bound, pieces=(), kind=jnp.bfloat16):
    entries = jax.random.normal(rng, extent, jnp.float32) * scale
    if len(pieces) > 0:
        entries = steps_of(rng, extent, pieces, -0.22, 0.18) * entries
    return jnp.clip(entries, min=-bound, max=bound).astype(kind)


def setup_inputs(seed: int = 0) -> dict:
    splits = jax.random.split(jax.random.key(seed), 8)
    acts = centred(splits[0], (TOTAL_ROWS, FF), 1.0, 6.0, ((0, 512),))
    grad_out = centred(splits[1], (TOTAL_ROWS, D), 0.04, 0.25, ((0, 512),))
    live_rows = draw_live_rows(jax.random.fold_in(splits[7], 71), 0)
    placement = draw_placement(jax.random.fold_in(splits[7], 71), 0)
    master = centred(splits[4], (EXPERTS, FF, D), FF ** -0.5, 0.21875, ((0, 16), (1, 32)), jnp.float32)
    moment1 = centred(splits[5], (EXPERTS, FF, D), 0.5, 3.0, ((0, 16), (1, 32)), jnp.float32)
    moment2 = jnp.clip(jnp.exp(math.log(5.0) - 4.6051702 * jax.random.uniform(splits[6], (EXPERTS, FF, D), jnp.float32) ** steps_of(splits[6], (EXPERTS, FF, D), ((0, 16), (1, 32)), -0.2, 0.2)), 0.05, 5.0)
    return dict(acts=acts, grad_out=grad_out, live_rows=live_rows, placement=placement, master=master, moment1=moment1, moment2=moment2)


beta_first = 0.9
beta_second = 0.95
learn_rate = 0.02
decay_rate = 0.1
epsilon = 1e-08
correct_first = 1.0 - (0.9 ** 50) ** 2
correct_second = 1.0 - (0.95 ** 50) ** 2

def reference(acts, grad_out, live_rows, placement, master, moment1, moment2):
    half_weights = master.astype(jnp.bfloat16)
    act_blocks = acts.reshape(N_GROUP, N_DEV, ROWS, FF)
    out_blocks = grad_out.reshape(N_GROUP, N_DEV, ROWS, D)
    live_blocks = live_rows.reshape(N_GROUP, N_DEV)
    place_blocks = placement.reshape(N_GROUP, N_DEV)
    positions = jnp.arange(ROWS, dtype=jnp.int32)

    def per_device(partial_value, inputs):
        act_rows, out_rows, live_count, expert = inputs
        weight = lax.dynamic_index_in_dim(half_weights, expert, 0, keepdims=False)
        live_mask = (positions < live_count)[:, None]
        grad_rows = jnp.dot(out_rows, weight.T, preferred_element_type=jnp.float32)
        grad_rows = jnp.where(live_mask, grad_rows, jnp.zeros((), grad_rows.dtype)).astype(jnp.bfloat16)
        masked = jnp.where(live_mask, act_rows, jnp.zeros((), act_rows.dtype))
        copy_grad = jnp.dot(masked.T, out_rows, preferred_element_type=jnp.float32).astype(jnp.bfloat16)
        copy_grad = lax.optimization_barrier(copy_grad).astype(jnp.float32)
        current = lax.dynamic_index_in_dim(partial_value, expert, 0, keepdims=False)
        partial_value = lax.dynamic_update_index_in_dim(partial_value, current + copy_grad, expert, 0)
        return (partial_value, grad_rows)

    def per_group(total, inputs):
        partial_value = jnp.zeros((EXPERTS, FF, D), jnp.float32)
        partial_value, grad_rows = lax.scan(per_device, partial_value, inputs)
        rounded = lax.optimization_barrier(partial_value.astype(jnp.bfloat16)).astype(jnp.float32)
        return (total + rounded, grad_rows)
    total = jnp.zeros((EXPERTS, FF, D), jnp.float32)
    gradient, grad_rows = lax.scan(per_group, total, (act_blocks, out_blocks, live_blocks, place_blocks))
    grad_in = grad_rows.reshape(N_GROUP * N_DEV * ROWS, FF)
    new_moment1 = beta_first * moment1 + (1.0 - beta_first) * gradient
    new_moment2 = beta_second * moment2 + (1.0 - beta_second) * gradient * gradient
    ascent = new_moment1 / correct_first / (jnp.sqrt(new_moment2 / correct_second) + epsilon)
    new_master = master - learn_rate * (ascent + decay_rate * master)
    return (grad_in, new_master, new_moment1, new_moment2)
```

```python
import functools

import jax
import jax.numpy as jnp
from jax import lax
from jax.experimental import pallas as pl
from jax.experimental.pallas import tpu as pltpu
from jax.sharding import PartitionSpec as P

beta_first = 0.9
beta_second = 0.95
learn_rate = 0.02
decay_rate = 0.1
epsilon = 1e-08
correct_first = 1.0 - (0.9**50) ** 2
correct_second = 1.0 - (0.95**50) ** 2

MESH = pl.DeviceIdType.MESH
NX, NY, NZ = 4, 8, 8


def near_offsets():
    half = NY // 2
    near = half // 2
    both = (half - 1) // 2
    own = [(dx, dy) for dx in range(NX) for dy in range(-near, near + 1)]
    par = [(dx, dy) for dx in range(NX) for dy in range(-both, both + 1)]
    return own, par, near, both


def exchange_kernel(
    place_ref,
    tab_ref,
    half_ref,
    copy_ref,
    weight_ref,
    grad_ref,
    w_all,
    w_send_own,
    w_send_par,
    g_own,
    g_par,
    d_send,
    d_recv,
    r_send,
    r_recv,
    p_send,
    p_recv,
    pair_sem,
    ag_send_sem,
    ag_recv_sem,
    core_send_sem,
    core_recv_sem,
    gdev_send_sem,
    gdev_recv_sem,
    wdev_send_sem,
    wdev_recv_sem,
    d_sem,
    rs_send_sem,
    rs_recv_sem,
    local_sem,
):
    g = lax.axis_index("group")
    v = lax.axis_index("dev")
    z, c = g // 2, g % 2
    x, y = v // NY, v % NY
    half = NY // 2
    own, par, near, both = near_offsets()
    n_own, n_par = len(own), len(par)
    vp = x * NY + lax.rem(y + half, NY)
    members = NX * NY

    def at(dx, dy):
        return lax.rem(x + dx + NX, NX) * NY + lax.rem(y + dy + NY, NY)

    def pair_of(vd):
        return (vd // NY) * NY + lax.rem(vd % NY + half, NY)

    def zmod(k):
        return lax.rem(z + k + NZ, NZ)

    pair_dev = (g, vp)
    core_dev = (z * 2 + 1 - c, v)
    z_dev = ((zmod(1) * 2 + c, v), (zmod(-1) * 2 + c, v))

    def remote(src, dst, ssem, rsem, dev):
        return pltpu.make_async_remote_copy(
            src_ref=src, dst_ref=dst, send_sem=ssem, recv_sem=rsem, device_id=dev, device_id_type=MESH
        )

    barrier = pltpu.get_barrier_semaphore()
    peers = [(g, at(dx, dy)) for dx, dy in own if (dx, dy) != (0, 0)] + [pair_dev, core_dev]
    if NZ > 1:
        peers += list(z_dev)
    for dev in peers:
        pl.semaphore_signal(barrier, inc=1, device_id=dev, device_id_type=MESH)

    zero = jnp.zeros(half_ref.shape[1:], jnp.bfloat16)
    g_own[n_own] = zero
    g_par[n_par] = zero
    d_recv[0, NZ] = zero
    d_recv[1, NZ] = zero

    local = [
        pltpu.make_async_copy(half_ref, w_all.at[0, pl.ds(2 * g, 2)], local_sem.at[0]),
        pltpu.make_async_copy(copy_ref.at[v], g_own.at[own.index((0, 0))], local_sem.at[1]),
        pltpu.make_async_copy(copy_ref.at[vp], g_par.at[par.index((0, 0))], local_sem.at[2]),
    ]
    for cp in local:
        cp.start()
    pl.semaphore_wait(barrier, len(peers))

    sends = []

    def go(cp):
        cp.start()
        sends.append(cp)

    block = pl.ds(2 * g, 2)
    pair_copy = remote(half_ref, w_all.at[1, block], pair_sem.at[0], pair_sem.at[1], pair_dev)
    go(pair_copy)
    hops = ((NZ // 2, (NZ - 1) // 2), ((NZ - 1) // 2, NZ // 2))

    def ag(ring, way, step, src=None):
        k = step - 1
        o = zmod(-k if way == 0 else k) * 2 + c
        part = w_all.at[ring, pl.ds(2 * o, 2)]
        return remote(
            part if src is None else src,
            part,
            ag_send_sem.at[ring, way, k],
            ag_recv_sem.at[ring, way, k],
            z_dev[way],
        )

    def ag_arrived(ring, way, step):
        o = zmod(-step if way == 0 else step) * 2 + c
        part = w_all.at[ring, pl.ds(2 * o, 2)]
        remote(
            part, part, ag_send_sem.at[ring, way, step - 1], ag_recv_sem.at[ring, way, step - 1], z_dev[way]
        ).wait_recv()

    def core_copy(ring, k, src=None):
        o = zmod(-k) * 2 + c
        part = w_all.at[ring, pl.ds(2 * o, 2)]
        return remote(
            part if src is None else src,
            part,
            core_send_sem.at[ring, k],
            core_recv_sem.at[ring, k],
            core_dev,
        )

    def core_arrived(ring, k):
        o = zmod(-k) * 2 + 1 - c
        part = w_all.at[ring, pl.ds(2 * o, 2)]
        remote(part, part, core_send_sem.at[ring, k], core_recv_sem.at[ring, k], core_dev).wait_recv()

    def launch(ring, src):
        for way in (0, 1):
            if hops[ring][way] > 0:
                go(ag(ring, way, 1, src))
        go(core_copy(ring, 0, src))

    def forward(ring, step):
        for way in (0, 1):
            if step <= hops[ring][way]:
                ag_arrived(ring, way, step)
                if step < hops[ring][way]:
                    go(ag(ring, way, step + 1))
                go(core_copy(ring, step if way == 0 else NZ - step))

    launch(0, half_ref)

    g_waits = []

    def g_go(src, dst, s, dev):
        cp = remote(src, dst, gdev_send_sem.at[s], gdev_recv_sem.at[s], dev)
        go(cp)
        g_waits.append(cp)

    order = sorted(own, key=lambda d: (-(min(d[0], NX - d[0]) + abs(d[1])), d))
    for dx, dy in order:
        if (dx, dy) == (0, 0):
            continue
        vd = at(dx, dy)
        s = own.index((dx, dy))
        g_go(copy_ref.at[vd], g_own.at[s], s, (g, vd))
        if (dx, dy) in par:
            s = par.index((dx, dy))
            g_go(copy_ref.at[pair_of(vd)], g_par.at[s], n_own + s, (g, vd))

    steps = NZ // 2
    early = min(2, steps)
    for k in range(1, early + 1):
        forward(0, k)
    pair_copy.wait_recv()
    launch(1, None)
    for k in range(early + 1, steps + 1):
        forward(0, k)
        forward(1, k - early)
    for k in range(max(1, steps - early + 1), steps + 1):
        forward(1, k)
    for cp in local:
        cp.wait()
    for ring in (0, 1):
        for k in range(NZ):
            core_arrived(ring, k)

    w_waits = []

    def w_go(src, dst, s, dev):
        cp = remote(src, dst, wdev_send_sem.at[s], wdev_recv_sem.at[s], dev)
        go(cp)
        w_waits.append(cp)

    for dx, dy in order:
        vd = at(dx, dy)
        e = place_ref[g * members + vd]
        if (dx, dy) == (0, 0):
            weight_ref[v] = w_all[0, e]
            weight_ref[vp] = w_all[1, e]
            continue
        s = own.index((dx, dy))
        w_send_own[s] = w_all[0, e]
        w_go(w_send_own.at[s], weight_ref.at[v], s, (g, vd))
        if (dx, dy) in par:
            s = par.index((dx, dy))
            w_send_par[s] = w_all[1, e]
            w_go(w_send_par.at[s], weight_ref.at[vp], n_own + s, (g, vd))

    for cp in g_waits:
        cp.wait_recv()
    recv = (g_own, g_par)
    d_waits = []
    for h in (1, 0):

        def owner_sum(zz, carry, h=h):
            o = 2 * zz + 1 - c
            first = recv[h][tab_ref[2 * h, o]].astype(jnp.float32)
            second = recv[h][tab_ref[2 * h + 1, o]].astype(jnp.float32)
            d_send[h, zz] = (first + second).astype(jnp.bfloat16)
            return carry

        lax.fori_loop(0, NZ, owner_sum, 0)
        cp = remote(d_send.at[h], d_recv.at[h, pl.ds(0, NZ)], d_sem.at[0, h], d_sem.at[1, h], core_dev)
        go(cp)
        d_waits.append(cp)
    for cp in d_waits:
        cp.wait_recv()

    def chip_sum(h, zt, j):
        e = 2 * (2 * zt + c) + j
        first = recv[h][tab_ref[4 + 2 * h, e]].astype(jnp.float32)
        second = recv[h][tab_ref[5 + 2 * h, e]].astype(jnp.float32)
        return first + second + d_recv[h, tab_ref[8, e]].astype(jnp.float32)

    def rs(h, way, step):
        return remote(
            r_send.at[h, way, step - 1],
            r_recv.at[h, way, step - 1],
            rs_send_sem.at[h, way, step - 1],
            rs_recv_sem.at[h, way, step - 1],
            z_dev[1 - way],
        )

    def rs_step(h, step):
        for way in (0, 1):
            length = hops[h][way]
            if step > length:
                continue
            away = length - step + 1
            zt = zmod(-away if way == 0 else away)
            if step > 1:
                rs(h, way, step - 1).wait_recv()
            for j in (0, 1):
                total = chip_sum(h, zt, j)
                if step > 1:
                    total = total + r_recv[h, way, step - 2, j].astype(jnp.float32)
                r_send[h, way, step - 1, j] = total.astype(jnp.bfloat16)
            go(rs(h, way, step))

    def rs_last(h):
        for way in (0, 1):
            if hops[h][way] > 0:
                rs(h, way, hops[h][way]).wait_recv()

    def home_sum(h, j):
        total = chip_sum(h, z, j)
        for way in (0, 1):
            if hops[h][way] > 0:
                total = total + r_recv[h, way, hops[h][way] - 1, j].astype(jnp.float32)
        return total

    for step in range(1, steps + 1):
        rs_step(1, step)
        rs_step(0, step)
    rs_last(1)
    for j in (0, 1):
        p_send[j] = home_sum(1, j).astype(jnp.bfloat16)
    back = remote(p_send, p_recv, pair_sem.at[2], pair_sem.at[3], pair_dev)
    go(back)
    rs_last(0)
    back.wait_recv()
    for j in (0, 1):
        grad_ref[j] = home_sum(0, j) + p_recv[j].astype(jnp.float32)

    for cp in w_waits:
        cp.wait_recv()
    for cp in sends:
        cp.wait_send()


def exchange(placement, table, half_weights, copy_grad):
    rows, width = half_weights.shape[1:]
    own, par, _, _ = near_offsets()
    n_own, n_par = len(own), len(par)
    owners = 2 * NZ
    steps = max(1, NZ // 2)
    dma = pltpu.SemaphoreType.DMA
    vmem = pl.BlockSpec(memory_space=pltpu.VMEM)
    smem = pl.BlockSpec(memory_space=pltpu.SMEM)

    def blocks(*lead):
        return pltpu.VMEM(lead + (rows, width), jnp.bfloat16)

    return pl.pallas_call(
        exchange_kernel,
        name="exchange",
        out_shape=(
            jax.ShapeDtypeStruct((NX * NY, rows, width), jnp.bfloat16),
            jax.ShapeDtypeStruct((2, rows, width), jnp.float32),
        ),
        in_specs=[smem, smem, vmem, vmem],
        out_specs=(vmem, vmem),
        scratch_shapes=[
            blocks(2, 2 * owners),
            blocks(n_own),
            blocks(n_par),
            blocks(n_own + 1),
            blocks(n_par + 1),
            blocks(2, NZ),
            blocks(2, NZ + 1),
            blocks(2, 2, steps, 2),
            blocks(2, 2, steps, 2),
            blocks(2),
            blocks(2),
            dma((4,)),
            dma((2, 2, steps)),
            dma((2, 2, steps)),
            dma((2, NZ)),
            dma((2, NZ)),
            dma((n_own + n_par,)),
            dma((n_own + n_par,)),
            dma((n_own + n_par,)),
            dma((n_own + n_par,)),
            dma((2, 2)),
            dma((2, 2, steps)),
            dma((2, 2, steps)),
            dma((3,)),
        ],
        compiler_params=pltpu.CompilerParams(
            collective_id=0, has_side_effects=True, vmem_limit_bytes=60 * 2**20
        ),
    )(placement, table, half_weights, copy_grad)


def adam_update(master, moment1, moment2, gradient):
    new_moment1 = beta_first * moment1 + (1.0 - beta_first) * gradient
    new_moment2 = beta_second * moment2 + (1.0 - beta_second) * gradient * gradient
    ascent = new_moment1 / correct_first / (jnp.sqrt(new_moment2 / correct_second) + epsilon)
    new_master = master - learn_rate * (ascent + decay_rate * master)
    return (new_master, new_moment1, new_moment2)


def slot_table(placement):
    own, par, near, both = near_offsets()
    g = lax.axis_index("group")
    v = lax.axis_index("dev")
    x, y = v // NY, v % NY
    members = NX * NY
    owners = 2 * NZ
    everyone = placement.reshape(2 * NZ, members)
    roster = lax.dynamic_index_in_dim(everyone, g, 0, keepdims=False)
    other = lax.dynamic_index_in_dim(everyone, g + 1 - 2 * (g % 2), 0, keepdims=False)
    experts = lax.iota(jnp.int32, 2 * owners)
    spots = lax.iota(jnp.int32, members)[None, :]
    owned = roster[None, :] // 2 == experts[:, None] // 2
    first = jnp.min(jnp.where(owned, spots, members), axis=1)
    second = jnp.max(jnp.where(owned, spots, -1), axis=1)
    runs = jnp.any(roster[None, :] == experts[:, None], axis=1)
    other_runs = jnp.any(other[None, :] == experts[:, None], axis=1)

    def slot(source, reach, none):
        dx = (x - source // NY + NX) % NX
        dy = (y - source % NY + NY + NY // 2) % NY - NY // 2
        found = (dy <= reach) & (dy >= -reach)
        return jnp.where(found, dx * (2 * reach + 1) + dy + reach, none)

    per_owner = jnp.stack(
        [slot(first, near, len(own)), slot(second, near, len(own)), slot(first, both, len(par)), slot(second, both, len(par))]
    )
    none = jnp.array([len(own), len(own), len(par), len(par)], jnp.int32)[:, None]
    per_expert = jnp.where(runs[None, :], per_owner, none)
    beside = jnp.where(other_runs, experts // 4, NZ)
    by_owner = jnp.pad(per_owner[:, ::2], ((0, 0), (0, owners)))
    return jnp.concatenate([by_owner, per_expert, beside[None, :]], axis=0)


def on_device(acts, grad_out, live_rows, placement, master, moment1, moment2):
    half_weights = master.astype(jnp.bfloat16)
    live_mask = (lax.iota(jnp.int32, acts.shape[0]) < live_rows[0])[:, None]
    masked_acts = jnp.where(live_mask, acts, jnp.zeros((), jnp.bfloat16))
    copy_grad = lax.dot_general(
        masked_acts, grad_out, (((0,), (0,)), ((), ())), preferred_element_type=jnp.float32
    ).astype(jnp.bfloat16)
    members = NX * NY
    incoming, gradient = exchange(
        placement,
        slot_table(placement),
        half_weights,
        copy_grad.reshape(members, -1, copy_grad.shape[-1]),
    )
    full_weight = incoming.reshape(-1, incoming.shape[-1])
    grad_rows = lax.dot_general(
        grad_out, full_weight, (((1,), (1,)), ((), ())), preferred_element_type=jnp.float32
    )
    grad_in = jnp.where(live_mask, grad_rows, jnp.zeros((), jnp.float32)).astype(jnp.bfloat16)
    new_master, new_moment1, new_moment2 = adam_update(master, moment1, moment2, gradient)
    return (grad_in, new_master, new_moment1, new_moment2)


def solution(mesh):
    in_specs = (
        P(("group", "dev"), None),
        P(("group", "dev"), None),
        P(("group", "dev")),
        P(),
        P("group", "dev", None),
        P("group", "dev", None),
        P("group", "dev", None),
    )
    out_specs = (
        P(("group", "dev"), None),
        P("group", "dev", None),
        P("group", "dev", None),
        P("group", "dev", None),
    )
    return jax.shard_map(
        on_device, mesh=mesh, in_specs=in_specs, out_specs=out_specs, check_vma=False
    )
```

```python
import functools

import jax
import jax.numpy as jnp
from jax import lax
from jax.experimental import pallas as pl
from jax.experimental.pallas import tpu as pltpu
from jax.sharding import PartitionSpec as P

beta_first = 0.9
beta_second = 0.95
learn_rate = 0.02
decay_rate = 0.1
epsilon = 1e-08
correct_first = 1.0 - (0.9**50) ** 2
correct_second = 1.0 - (0.95**50) ** 2

MESH = pl.DeviceIdType.MESH
NX, NY, NZ = 4, 8, 8


def near_offsets():
    half = NY // 2
    near = half // 2
    both = (half - 1) // 2
    own = [(dx, dy) for dx in range(NX) for dy in range(-near, near + 1)]
    par = [(dx, dy) for dx in range(NX) for dy in range(-both, both + 1)]
    return own, par, near, both


def step_kernel(
    place_ref,
    tab_ref,
    live_ref,
    acts_ref,
    out_ref,
    master_ref,
    rows_ref,
    grad_ref,
    half_w,
    copy_g,
    weight,
    in_parts,
    w_own,
    w_par,
    w_send_own,
    w_send_par,
    g_own,
    g_par,
    d_send,
    d_own,
    d_par,
    r_send,
    r_recv,
    p_send,
    p_recv,
    pair_sem,
    ag_send_sem,
    ag_recv_sem,
    core_send_sem,
    core_recv_sem,
    gdev_send_sem,
    gdev_recv_sem,
    wdev_send_sem,
    wdev_recv_sem,
    d_sem,
    rs_send_sem,
    rs_recv_sem,
    local_sem,
):
    g = lax.axis_index("group")
    v = lax.axis_index("dev")
    z, c = g // 2, g % 2
    x, y = v // NY, v % NY
    half = NY // 2
    own, par, near, both = near_offsets()
    n_own, n_par = len(own), len(par)
    vp = x * NY + lax.rem(y + half, NY)
    members = NX * NY
    rows, width = half_w.shape[1:]
    w_all, d_recv = (w_own, w_par), (d_own, d_par)

    def at(dx, dy):
        return lax.rem(x + dx + NX, NX) * NY + lax.rem(y + dy + NY, NY)

    def pair_of(vd):
        return (vd // NY) * NY + lax.rem(vd % NY + half, NY)

    def zmod(k):
        return lax.rem(z + k + NZ, NZ)

    pair_dev = (g, vp)
    core_dev = (z * 2 + 1 - c, v)
    z_dev = ((zmod(1) * 2 + c, v), (zmod(-1) * 2 + c, v))

    def remote(src, dst, ssem, rsem, dev):
        return pltpu.make_async_remote_copy(
            src_ref=src, dst_ref=dst, send_sem=ssem, recv_sem=rsem, device_id=dev, device_id_type=MESH
        )

    barrier = pltpu.get_barrier_semaphore()
    peers = [(g, at(dx, dy)) for dx, dy in own if (dx, dy) != (0, 0)] + [pair_dev, core_dev]
    if NZ > 1:
        peers += list(z_dev)
    for dev in peers:
        pl.semaphore_signal(barrier, inc=1, device_id=dev, device_id_type=MESH)

    half_w[...] = master_ref[...].astype(jnp.bfloat16)
    zero = jnp.zeros((rows, width), jnp.bfloat16)
    g_own[n_own] = zero
    g_par[n_par] = zero
    d_own[NZ] = zero
    d_par[NZ] = zero
    pl.semaphore_wait(barrier, len(peers))

    sends = []

    def go(cp):
        cp.start()
        sends.append(cp)

    block = pl.ds(2 * g, 2)
    pair_copy = remote(half_w, w_all[1].at[block], pair_sem.at[0], pair_sem.at[1], pair_dev)
    go(pair_copy)
    hops = ((NZ // 2, (NZ - 1) // 2), ((NZ - 1) // 2, NZ // 2))

    def ag(ring, way, step, src=None):
        k = step - 1
        o = zmod(-k if way == 0 else k) * 2 + c
        part = w_all[ring].at[pl.ds(2 * o, 2)]
        return remote(
            part if src is None else src,
            part,
            ag_send_sem.at[ring, way, k],
            ag_recv_sem.at[ring, way, k],
            z_dev[way],
        )

    def ag_arrived(ring, way, step):
        o = zmod(-step if way == 0 else step) * 2 + c
        part = w_all[ring].at[pl.ds(2 * o, 2)]
        remote(
            part, part, ag_send_sem.at[ring, way, step - 1], ag_recv_sem.at[ring, way, step - 1], z_dev[way]
        ).wait_recv()

    def core_copy(ring, k, src=None):
        o = zmod(-k) * 2 + c
        part = w_all[ring].at[pl.ds(2 * o, 2)]
        return remote(
            part if src is None else src,
            part,
            core_send_sem.at[ring, k],
            core_recv_sem.at[ring, k],
            core_dev,
        )

    def core_arrived(ring):
        for k in range(NZ):
            o = zmod(-k) * 2 + 1 - c
            part = w_all[ring].at[pl.ds(2 * o, 2)]
            remote(part, part, core_send_sem.at[ring, k], core_recv_sem.at[ring, k], core_dev).wait_recv()

    def launch(ring, src):
        for way in (0, 1):
            if hops[ring][way] > 0:
                go(ag(ring, way, 1, src))
        go(core_copy(ring, 0, src))

    def forward(ring, step):
        for way in (0, 1):
            if 1 <= step <= hops[ring][way]:
                ag_arrived(ring, way, step)
                if step < hops[ring][way]:
                    go(ag(ring, way, step + 1))
                go(core_copy(ring, step if way == 0 else NZ - step))

    launch(0, half_w)
    local_w = pltpu.make_async_copy(half_w, w_all[0].at[block], local_sem.at[0])
    local_w.start()

    live = lax.broadcasted_iota(jnp.int32, acts_ref.shape, 0) < live_ref[0]
    masked = jnp.where(live, acts_ref[...], jnp.zeros((), jnp.bfloat16))
    strip = min(512, width)

    def copy_strip(i, carry):
        cols = pl.ds(pl.multiple_of(i * strip, strip), strip)
        product = lax.dot_general(
            masked, out_ref[:, cols], (((0,), (0,)), ((), ())), preferred_element_type=jnp.float32
        )
        copy_g[:, :, cols] = product.astype(jnp.bfloat16).reshape(members, rows, strip)
        return carry

    lax.fori_loop(0, width // strip, copy_strip, 0)

    local_g = [
        pltpu.make_async_copy(copy_g.at[v], g_own.at[own.index((0, 0))], local_sem.at[1]),
        pltpu.make_async_copy(copy_g.at[vp], g_par.at[par.index((0, 0))], local_sem.at[2]),
    ]
    for cp in local_g:
        cp.start()
    g_waits = ([], [])

    def g_go(h, src, dst, s, dev):
        cp = remote(src, dst, gdev_send_sem.at[s], gdev_recv_sem.at[s], dev)
        go(cp)
        g_waits[h].append(cp)

    order = sorted(own, key=lambda d: (-(min(d[0], NX - d[0]) + abs(d[1])), d))
    order = [d for d in order if d != (0, 0)]
    for dx, dy in order:
        if (dx, dy) in par:
            vd = at(dx, dy)
            s = par.index((dx, dy))
            g_go(1, copy_g.at[pair_of(vd)], g_par.at[s], n_own + s, (g, vd))
    for dx, dy in order:
        vd = at(dx, dy)
        s = own.index((dx, dy))
        g_go(0, copy_g.at[vd], g_own.at[s], s, (g, vd))

    w_waits = {}

    def w_go(src, dst, s, dev, dx):
        cp = remote(src, dst, wdev_send_sem.at[s], wdev_recv_sem.at[s], dev)
        go(cp)
        w_waits.setdefault(dx, []).append(cp)

    def deal_own():
        for dx, dy in order:
            vd = at(dx, dy)
            s = own.index((dx, dy))
            w_send_own[s] = w_all[0][place_ref[g * members + vd]]
            w_go(w_send_own.at[s], weight.at[v], s, (g, vd), dx)
        weight[v] = w_all[0][place_ref[g * members + v]]

    def deal_par():
        for dx, dy in order:
            if (dx, dy) in par:
                vd = at(dx, dy)
                s = par.index((dx, dy))
                w_send_par[s] = w_all[1][place_ref[g * members + vd]]
                w_go(w_send_par.at[s], weight.at[vp], n_own + s, (g, vd), dx)
        weight[vp] = w_all[1][place_ref[g * members + v]]

    recv = (g_own, g_par)

    def core_swap(h):
        return remote(d_send.at[h], d_recv[h].at[pl.ds(0, NZ)], d_sem.at[0, h], d_sem.at[1, h], core_dev)

    def give_core(h):
        local_g[h].wait()
        for cp in g_waits[h]:
            cp.wait_recv()

        def owner_sum(zz, carry):
            e = 2 * (2 * zz + 1 - c)
            first = recv[h][tab_ref[4 * h, e]].astype(jnp.float32)
            second = recv[h][tab_ref[4 * h + 1, e]].astype(jnp.float32)
            d_send[h, zz] = (first + second).astype(jnp.bfloat16)
            return carry

        lax.fori_loop(0, NZ, owner_sum, 0)
        go(core_swap(h))

    def chip_sum(h, zt, j):
        e = 2 * (2 * zt + c) + j
        first = recv[h][tab_ref[4 * h + 2, e]].astype(jnp.float32)
        second = recv[h][tab_ref[4 * h + 3, e]].astype(jnp.float32)
        return first + second + d_recv[h][tab_ref[8, e]].astype(jnp.float32)

    def rs(h, way, step):
        return remote(
            r_send.at[h, way, step - 1],
            r_recv.at[h, way, step - 1],
            rs_send_sem.at[h, way, step - 1],
            rs_recv_sem.at[h, way, step - 1],
            z_dev[1 - way],
        )

    def rs_step(h, step):
        for way in (0, 1):
            length = hops[h][way]
            if step > length:
                continue
            away = length - step + 1
            zt = zmod(-away if way == 0 else away)
            if step > 1:
                rs(h, way, step - 1).wait_recv()
            for j in (0, 1):
                total = chip_sum(h, zt, j)
                if step > 1:
                    total = total + r_recv[h, way, step - 2, j].astype(jnp.float32)
                r_send[h, way, step - 1, j] = total.astype(jnp.bfloat16)
            go(rs(h, way, step))

    def rs_last(h):
        for way in (0, 1):
            if hops[h][way] > 0:
                rs(h, way, hops[h][way]).wait_recv()

    def home_sum(h, j):
        total = chip_sum(h, z, j)
        for way in (0, 1):
            if hops[h][way] > 0:
                total = total + r_recv[h, way, hops[h][way] - 1, j].astype(jnp.float32)
        return total

    steps = NZ // 2
    forward(0, 1)
    forward(0, 2)
    pair_copy.wait_recv()
    launch(1, None)
    forward(0, 3)
    forward(1, 1)
    give_core(1)
    for k in range(4, steps + 1):
        forward(0, k)
    forward(1, 2)
    core_swap(1).wait_recv()
    rs_step(1, 1)
    local_w.wait()
    core_arrived(0)
    deal_own()
    forward(1, 3)
    rs_step(1, 2)
    for k in range(4, steps + 1):
        forward(1, k)
    core_arrived(1)
    deal_par()
    rs_step(1, 3)
    give_core(0)
    for step in range(4, steps + 1):
        rs_step(1, step)
    core_swap(0).wait_recv()
    rs_step(0, 1)
    rs_last(1)
    for j in (0, 1):
        p_send[j] = home_sum(1, j).astype(jnp.bfloat16)
    back = remote(p_send, p_recv, pair_sem.at[2], pair_sem.at[3], pair_dev)
    go(back)
    for step in range(2, steps + 1):
        rs_step(0, step)
    rs_last(0)
    back.wait_recv()
    for j in (0, 1):
        grad_ref[j] = home_sum(0, j) + p_recv[j].astype(jnp.float32)

    for dx in sorted(range(NX), key=lambda d: (min(d, NX - d), d)):
        for cp in w_waits.get(dx, []):
            cp.wait_recv()
        xs = lax.rem(x - dx + NX, NX)
        part = weight[pl.ds(xs * NY, NY)].reshape(NY * rows, width)
        in_parts[xs] = lax.dot_general(
            out_ref[...], part, (((1,), (1,)), ((), ())), preferred_element_type=jnp.float32
        ).astype(jnp.bfloat16)
    for xs in range(NX):
        rows_ref[:, xs * NY * rows : (xs + 1) * NY * rows] = in_parts[xs]
    for cp in sends:
        cp.wait_send()


def step(placement, table, live_rows, acts, grad_out, master):
    rows, width = master.shape[1:]
    own, par, _, _ = near_offsets()
    n_own, n_par = len(own), len(par)
    owners = 2 * NZ
    steps = max(1, NZ // 2)
    dma = pltpu.SemaphoreType.DMA
    vmem = pl.BlockSpec(memory_space=pltpu.VMEM)
    smem = pl.BlockSpec(memory_space=pltpu.SMEM)

    def blocks(*lead):
        return pltpu.VMEM(lead + (rows, width), jnp.bfloat16)

    return pl.pallas_call(
        step_kernel,
        name="step",
        out_shape=(
            jax.ShapeDtypeStruct(acts.shape, jnp.bfloat16),
            jax.ShapeDtypeStruct(master.shape, jnp.float32),
        ),
        in_specs=[smem, smem, smem, vmem, vmem, vmem],
        out_specs=(vmem, vmem),
        scratch_shapes=[
            blocks(2),
            blocks(NX * NY),
            blocks(NX * NY),
            pltpu.VMEM((NX, acts.shape[0], NY * rows), jnp.bfloat16),
            blocks(2 * owners),
            blocks(2 * owners),
            blocks(n_own),
            blocks(n_par),
            blocks(n_own + 1),
            blocks(n_par + 1),
            blocks(2, NZ),
            blocks(NZ + 1),
            blocks(NZ + 1),
            blocks(2, 2, steps, 2),
            blocks(2, 2, steps, 2),
            blocks(2),
            blocks(2),
            dma((4,)),
            dma((2, 2, steps)),
            dma((2, 2, steps)),
            dma((2, NZ)),
            dma((2, NZ)),
            dma((n_own + n_par,)),
            dma((n_own + n_par,)),
            dma((n_own + n_par,)),
            dma((n_own + n_par,)),
            dma((2, 2)),
            dma((2, 2, steps)),
            dma((2, 2, steps)),
            dma((3,)),
        ],
        compiler_params=pltpu.CompilerParams(
            collective_id=0, has_side_effects=True, vmem_limit_bytes=60 * 2**20
        ),
    )(placement, table, live_rows, acts, grad_out, master)


def adam_update(master, moment1, moment2, gradient):
    new_moment1 = beta_first * moment1 + (1.0 - beta_first) * gradient
    new_moment2 = beta_second * moment2 + (1.0 - beta_second) * gradient * gradient
    ascent = new_moment1 / correct_first / (jnp.sqrt(new_moment2 / correct_second) + epsilon)
    new_master = master - learn_rate * (ascent + decay_rate * master)
    return (new_master, new_moment1, new_moment2)


def slot_table(placement):
    own, par, near, both = near_offsets()
    g = lax.axis_index("group")
    v = lax.axis_index("dev")
    x, y = v // NY, v % NY
    members = NX * NY
    experts = 4 * NZ
    roster = lax.dynamic_slice_in_dim(placement, g * members, members)
    other = lax.dynamic_slice_in_dim(placement, (g + 1 - 2 * (g % 2)) * members, members)
    shape = (9, experts, members)
    kind = lax.broadcasted_iota(jnp.int32, shape, 0)
    expert = lax.broadcasted_iota(jnp.int32, shape, 1)
    source = lax.broadcasted_iota(jnp.int32, shape, 2)
    dx = (x - source // NY + NX) % NX
    dy = (y - source % NY + NY + NY // 2) % NY - NY // 2
    reach = jnp.where(kind < 4, near, both)
    none = jnp.where(kind < 4, len(own), len(par))
    slot = jnp.where((dy <= reach) & (dy >= -reach), dx * (2 * reach + 1) + dy + reach, none)
    value = jnp.where(kind == 8, expert // 4, jnp.where(kind % 2 == 0, slot, -slot))
    runs = jnp.where(kind == 8, other[None, None, :], roster[None, None, :])
    match = jnp.where(kind % 4 < 2, (runs // 2 == expert // 2) & (kind < 8), False) | (runs == expert)
    best = jnp.max(jnp.where(match, value, -1000), axis=2)
    row = lax.broadcasted_iota(jnp.int32, shape[:2], 0)
    absent = jnp.where(row < 4, len(own), jnp.where(row < 8, len(par), NZ))
    return jnp.where(best == -1000, absent, jnp.abs(best))


def on_device(acts, grad_out, live_rows, placement, master, moment1, moment2):
    grad_rows, gradient = step(placement, slot_table(placement), live_rows, acts, grad_out, master)
    live_mask = (lax.iota(jnp.int32, acts.shape[0]) < live_rows[0])[:, None]
    grad_in = jnp.where(live_mask, grad_rows, jnp.zeros((), jnp.bfloat16))
    new_master, new_moment1, new_moment2 = adam_update(master, moment1, moment2, gradient)
    return (grad_in, new_master, new_moment1, new_moment2)


def solution(mesh):
    in_specs = (
        P(("group", "dev"), None),
        P(("group", "dev"), None),
        P(("group", "dev")),
        P(),
        P("group", "dev", None),
        P("group", "dev", None),
        P("group", "dev", None),
    )
    out_specs = (
        P(("group", "dev"), None),
        P("group", "dev", None),
        P("group", "dev", None),
        P("group", "dev", None),
    )
    return jax.shard_map(
        on_device, mesh=mesh, in_specs=in_specs, out_specs=out_specs, check_vma=False
    )
```

```python
import functools

import jax
import jax.numpy as jnp
from jax import lax
from jax.experimental import pallas as pl
from jax.experimental.pallas import tpu as pltpu
from jax.sharding import PartitionSpec as P

beta_first = 0.9
beta_second = 0.95
learn_rate = 0.02
decay_rate = 0.1
epsilon = 1e-08
correct_first = 1.0 - (0.9**50) ** 2
correct_second = 1.0 - (0.95**50) ** 2

MESH = pl.DeviceIdType.MESH
NX, NY, NZ = 4, 8, 8


def near_offsets():
    half = NY // 2
    near = half // 2
    both = (half - 1) // 2
    own = [(dx, dy) for dx in range(NX) for dy in range(-near, near + 1)]
    par = [(dx, dy) for dx in range(NX) for dy in range(-both, both + 1)]
    return own, par, near, both


def step_kernel(
    place_ref,
    tab_ref,
    live_ref,
    acts_hbm,
    out_hbm,
    master_hbm,
    rows_ref,
    grad_ref,
    acts_ref,
    out_ref,
    master_ref,
    half_w,
    copy_g,
    weight,
    in_parts,
    w_own,
    w_par,
    w_send_own,
    w_send_par,
    g_own,
    g_par,
    d_send,
    d_own,
    d_par,
    r_send,
    r_recv,
    p_send,
    p_recv,
    pair_sem,
    ag_send_sem,
    ag_recv_sem,
    core_send_sem,
    core_recv_sem,
    gdev_send_sem,
    gdev_recv_sem,
    wdev_send_sem,
    wdev_recv_sem,
    d_sem,
    rs_send_sem,
    rs_recv_sem,
    local_sem,
):
    g = lax.axis_index("group")
    v = lax.axis_index("dev")
    z, c = g // 2, g % 2
    x, y = v // NY, v % NY
    half = NY // 2
    own, par, near, both = near_offsets()
    n_own, n_par = len(own), len(par)
    vp = x * NY + lax.rem(y + half, NY)
    members = NX * NY
    rows, width = half_w.shape[1:]
    w_all, d_recv = (w_own, w_par), (d_own, d_par)

    def at(dx, dy):
        return lax.rem(x + dx + NX, NX) * NY + lax.rem(y + dy + NY, NY)

    def pair_of(vd):
        return (vd // NY) * NY + lax.rem(vd % NY + half, NY)

    def zmod(k):
        return lax.rem(z + k + NZ, NZ)

    pair_dev = (g, vp)
    core_dev = (z * 2 + 1 - c, v)
    z_dev = ((zmod(1) * 2 + c, v), (zmod(-1) * 2 + c, v))

    def remote(src, dst, ssem, rsem, dev):
        return pltpu.make_async_remote_copy(
            src_ref=src, dst_ref=dst, send_sem=ssem, recv_sem=rsem, device_id=dev, device_id_type=MESH
        )

    fetches = [
        pltpu.make_async_copy(src, dst, local_sem.at[3 + i])
        for i, (src, dst) in enumerate(((master_hbm, master_ref), (acts_hbm, acts_ref), (out_hbm, out_ref)))
    ]
    for cp in fetches:
        cp.start()
    barrier = pltpu.get_barrier_semaphore()
    peers = [(g, at(dx, dy)) for dx, dy in own if (dx, dy) != (0, 0)] + [pair_dev, core_dev]
    if NZ > 1:
        peers += list(z_dev)
    for dev in peers:
        pl.semaphore_signal(barrier, inc=1, device_id=dev, device_id_type=MESH)

    zero = jnp.zeros((rows, width), jnp.bfloat16)
    g_own[n_own] = zero
    g_par[n_par] = zero
    d_own[NZ] = zero
    d_par[NZ] = zero
    fetches[0].wait()
    half_w[...] = master_ref[...].astype(jnp.bfloat16)
    pl.semaphore_wait(barrier, len(peers))

    sends = []

    def go(cp):
        cp.start()
        sends.append(cp)

    block = pl.ds(2 * g, 2)
    pair_copy = remote(half_w, w_all[1].at[block], pair_sem.at[0], pair_sem.at[1], pair_dev)
    go(pair_copy)
    hops = ((NZ // 2, (NZ - 1) // 2), ((NZ - 1) // 2, NZ // 2))

    def ag(ring, way, step, src=None):
        k = step - 1
        o = zmod(-k if way == 0 else k) * 2 + c
        part = w_all[ring].at[pl.ds(2 * o, 2)]
        return remote(
            part if src is None else src,
            part,
            ag_send_sem.at[ring, way, k],
            ag_recv_sem.at[ring, way, k],
            z_dev[way],
        )

    def ag_arrived(ring, way, step):
        o = zmod(-step if way == 0 else step) * 2 + c
        part = w_all[ring].at[pl.ds(2 * o, 2)]
        remote(
            part, part, ag_send_sem.at[ring, way, step - 1], ag_recv_sem.at[ring, way, step - 1], z_dev[way]
        ).wait_recv()

    def core_copy(ring, k, src=None):
        o = zmod(-k) * 2 + c
        part = w_all[ring].at[pl.ds(2 * o, 2)]
        return remote(
            part if src is None else src,
            part,
            core_send_sem.at[ring, k],
            core_recv_sem.at[ring, k],
            core_dev,
        )

    def core_arrived(ring):
        for k in range(NZ):
            o = zmod(-k) * 2 + 1 - c
            part = w_all[ring].at[pl.ds(2 * o, 2)]
            remote(part, part, core_send_sem.at[ring, k], core_recv_sem.at[ring, k], core_dev).wait_recv()

    def launch(ring, src):
        for way in (0, 1):
            if hops[ring][way] > 0:
                go(ag(ring, way, 1, src))
        go(core_copy(ring, 0, src))

    def forward(ring, step):
        for way in (0, 1):
            if 1 <= step <= hops[ring][way]:
                ag_arrived(ring, way, step)
                if step < hops[ring][way]:
                    go(ag(ring, way, step + 1))
                go(core_copy(ring, step if way == 0 else NZ - step))

    launch(0, half_w)
    local_w = pltpu.make_async_copy(half_w, w_all[0].at[block], local_sem.at[0])
    local_w.start()

    fetches[1].wait()
    fetches[2].wait()
    live = lax.broadcasted_iota(jnp.int32, acts_ref.shape, 0) < live_ref[0]
    masked = jnp.where(live, acts_ref[...], jnp.zeros((), jnp.bfloat16))
    strip = min(512, width)

    def copy_strip(i, carry):
        cols = pl.ds(pl.multiple_of(i * strip, strip), strip)
        product = lax.dot_general(
            masked, out_ref[:, cols], (((0,), (0,)), ((), ())), preferred_element_type=jnp.float32
        )
        copy_g[:, :, cols] = product.astype(jnp.bfloat16).reshape(members, rows, strip)
        return carry

    lax.fori_loop(0, width // strip, copy_strip, 0)

    local_g = [
        pltpu.make_async_copy(copy_g.at[v], g_own.at[own.index((0, 0))], local_sem.at[1]),
        pltpu.make_async_copy(copy_g.at[vp], g_par.at[par.index((0, 0))], local_sem.at[2]),
    ]
    for cp in local_g:
        cp.start()
    g_waits = ([], [])

    def g_go(h, src, dst, s, dev):
        cp = remote(src, dst, gdev_send_sem.at[s], gdev_recv_sem.at[s], dev)
        go(cp)
        g_waits[h].append(cp)

    order = sorted(own, key=lambda d: (-(min(d[0], NX - d[0]) + abs(d[1])), d))
    order = [d for d in order if d != (0, 0)]
    for dx, dy in order:
        if (dx, dy) in par:
            vd = at(dx, dy)
            s = par.index((dx, dy))
            g_go(1, copy_g.at[pair_of(vd)], g_par.at[s], n_own + s, (g, vd))
    for dx, dy in order:
        vd = at(dx, dy)
        s = own.index((dx, dy))
        g_go(0, copy_g.at[vd], g_own.at[s], s, (g, vd))

    w_waits = {}

    def w_go(src, dst, s, dev, dx):
        cp = remote(src, dst, wdev_send_sem.at[s], wdev_recv_sem.at[s], dev)
        go(cp)
        w_waits.setdefault(dx, []).append(cp)

    def deal_own():
        for dx, dy in order:
            vd = at(dx, dy)
            s = own.index((dx, dy))
            w_send_own[s] = w_all[0][place_ref[g * members + vd]]
            w_go(w_send_own.at[s], weight.at[v], s, (g, vd), dx)
        weight[v] = w_all[0][place_ref[g * members + v]]

    def deal_par():
        for dx, dy in order:
            if (dx, dy) in par:
                vd = at(dx, dy)
                s = par.index((dx, dy))
                w_send_par[s] = w_all[1][place_ref[g * members + vd]]
                w_go(w_send_par.at[s], weight.at[vp], n_own + s, (g, vd), dx)
        weight[vp] = w_all[1][place_ref[g * members + v]]

    recv = (g_own, g_par)

    def core_swap(h):
        return remote(d_send.at[h], d_recv[h].at[pl.ds(0, NZ)], d_sem.at[0, h], d_sem.at[1, h], core_dev)

    def give_core(h):
        local_g[h].wait()
        for cp in g_waits[h]:
            cp.wait_recv()

        def owner_sum(zz, carry):
            e = 2 * (2 * zz + 1 - c)
            first = recv[h][tab_ref[4 * h, e]].astype(jnp.float32)
            second = recv[h][tab_ref[4 * h + 1, e]].astype(jnp.float32)
            d_send[h, zz] = (first + second).astype(jnp.bfloat16)
            return carry

        lax.fori_loop(0, NZ, owner_sum, 0)
        go(core_swap(h))

    def chip_sum(h, zt, j):
        e = 2 * (2 * zt + c) + j
        first = recv[h][tab_ref[4 * h + 2, e]].astype(jnp.float32)
        second = recv[h][tab_ref[4 * h + 3, e]].astype(jnp.float32)
        return first + second + d_recv[h][tab_ref[8, e]].astype(jnp.float32)

    def rs(h, way, step):
        return remote(
            r_send.at[h, way, step - 1],
            r_recv.at[h, way, step - 1],
            rs_send_sem.at[h, way, step - 1],
            rs_recv_sem.at[h, way, step - 1],
            z_dev[1 - way],
        )

    def rs_step(h, step):
        for way in (0, 1):
            length = hops[h][way]
            if step > length:
                continue
            away = length - step + 1
            zt = zmod(-away if way == 0 else away)
            if step > 1:
                rs(h, way, step - 1).wait_recv()
            for j in (0, 1):
                total = chip_sum(h, zt, j)
                if step > 1:
                    total = total + r_recv[h, way, step - 2, j].astype(jnp.float32)
                r_send[h, way, step - 1, j] = total.astype(jnp.bfloat16)
            go(rs(h, way, step))

    def rs_last(h):
        for way in (0, 1):
            if hops[h][way] > 0:
                rs(h, way, hops[h][way]).wait_recv()

    def home_sum(h, j):
        total = chip_sum(h, z, j)
        for way in (0, 1):
            if hops[h][way] > 0:
                total = total + r_recv[h, way, hops[h][way] - 1, j].astype(jnp.float32)
        return total

    steps = NZ // 2
    forward(0, 1)
    forward(0, 2)
    pair_copy.wait_recv()
    launch(1, None)
    forward(0, 3)
    forward(1, 1)
    give_core(1)
    for k in range(4, steps + 1):
        forward(0, k)
    forward(1, 2)
    core_swap(1).wait_recv()
    rs_step(1, 1)
    local_w.wait()
    core_arrived(0)
    deal_own()
    forward(1, 3)
    rs_step(1, 2)
    for k in range(4, steps + 1):
        forward(1, k)
    core_arrived(1)
    deal_par()
    rs_step(1, 3)
    give_core(0)
    for step in range(4, steps + 1):
        rs_step(1, step)
    core_swap(0).wait_recv()
    rs_step(0, 1)
    rs_last(1)
    for j in (0, 1):
        p_send[j] = home_sum(1, j).astype(jnp.bfloat16)
    back = remote(p_send, p_recv, pair_sem.at[2], pair_sem.at[3], pair_dev)
    go(back)
    for step in range(2, steps + 1):
        rs_step(0, step)
    rs_last(0)

    kept = lax.broadcasted_iota(jnp.int32, (acts_ref.shape[0], NY * rows), 0) < live_ref[0]
    for i, dx in enumerate(sorted(range(NX), key=lambda d: (min(d, NX - d), d))):
        if i == NX - 1:
            back.wait_recv()
            for j in (0, 1):
                grad_ref[j] = home_sum(0, j) + p_recv[j].astype(jnp.float32)
        for cp in w_waits.get(dx, []):
            cp.wait_recv()
        xs = lax.rem(x - dx + NX, NX)
        part = weight[pl.ds(xs * NY, NY)].reshape(NY * rows, width)
        product = lax.dot_general(
            out_ref[...], part, (((1,), (1,)), ((), ())), preferred_element_type=jnp.float32
        )
        in_parts[xs] = jnp.where(kept, product, jnp.zeros((), jnp.float32)).astype(jnp.bfloat16)
    for xs in range(NX):
        rows_ref[:, xs * NY * rows : (xs + 1) * NY * rows] = in_parts[xs]
    for cp in sends:
        cp.wait_send()


def step(placement, table, live_rows, acts, grad_out, master):
    rows, width = master.shape[1:]
    own, par, _, _ = near_offsets()
    n_own, n_par = len(own), len(par)
    owners = 2 * NZ
    steps = max(1, NZ // 2)
    dma = pltpu.SemaphoreType.DMA
    vmem = pl.BlockSpec(memory_space=pltpu.VMEM)
    smem = pl.BlockSpec(memory_space=pltpu.SMEM)
    anywhere = pl.BlockSpec(memory_space=pl.ANY)

    def blocks(*lead):
        return pltpu.VMEM(lead + (rows, width), jnp.bfloat16)

    return pl.pallas_call(
        step_kernel,
        name="step",
        out_shape=(
            jax.ShapeDtypeStruct(acts.shape, jnp.bfloat16),
            jax.ShapeDtypeStruct(master.shape, jnp.float32),
        ),
        in_specs=[smem, smem, smem, anywhere, anywhere, anywhere],
        out_specs=(vmem, vmem),
        scratch_shapes=[
            pltpu.VMEM(acts.shape, acts.dtype),
            pltpu.VMEM(grad_out.shape, grad_out.dtype),
            pltpu.VMEM(master.shape, master.dtype),
            blocks(2),
            blocks(NX * NY),
            blocks(NX * NY),
            pltpu.VMEM((NX, acts.shape[0], NY * rows), jnp.bfloat16),
            blocks(2 * owners),
            blocks(2 * owners),
            blocks(n_own),
            blocks(n_par),
            blocks(n_own + 1),
            blocks(n_par + 1),
            blocks(2, NZ),
            blocks(NZ + 1),
            blocks(NZ + 1),
            blocks(2, 2, steps, 2),
            blocks(2, 2, steps, 2),
            blocks(2),
            blocks(2),
            dma((4,)),
            dma((2, 2, steps)),
            dma((2, 2, steps)),
            dma((2, NZ)),
            dma((2, NZ)),
            dma((n_own + n_par,)),
            dma((n_own + n_par,)),
            dma((n_own + n_par,)),
            dma((n_own + n_par,)),
            dma((2, 2)),
            dma((2, 2, steps)),
            dma((2, 2, steps)),
            dma((6,)),
        ],
        compiler_params=pltpu.CompilerParams(
            collective_id=0, has_side_effects=True, vmem_limit_bytes=60 * 2**20
        ),
    )(placement, table, live_rows, acts, grad_out, master)


def adam_update(master, moment1, moment2, gradient):
    new_moment1 = beta_first * moment1 + (1.0 - beta_first) * gradient
    new_moment2 = beta_second * moment2 + (1.0 - beta_second) * gradient * gradient
    ascent = new_moment1 / correct_first / (jnp.sqrt(new_moment2 / correct_second) + epsilon)
    new_master = master - learn_rate * (ascent + decay_rate * master)
    return (new_master, new_moment1, new_moment2)


def slot_table(placement):
    own, par, near, both = near_offsets()
    g = lax.axis_index("group")
    v = lax.axis_index("dev")
    x, y = v // NY, v % NY
    members = NX * NY
    experts = 4 * NZ
    roster = lax.dynamic_slice_in_dim(placement, g * members, members)
    other = lax.dynamic_slice_in_dim(placement, (g + 1 - 2 * (g % 2)) * members, members)
    shape = (9, experts, members)
    kind = lax.broadcasted_iota(jnp.int32, shape, 0)
    expert = lax.broadcasted_iota(jnp.int32, shape, 1)
    source = lax.broadcasted_iota(jnp.int32, shape, 2)
    dx = (x - source // NY + NX) % NX
    dy = (y - source % NY + NY + NY // 2) % NY - NY // 2
    reach = jnp.where(kind < 4, near, both)
    none = jnp.where(kind < 4, len(own), len(par))
    slot = jnp.where((dy <= reach) & (dy >= -reach), dx * (2 * reach + 1) + dy + reach, none)
    value = jnp.where(kind == 8, expert // 4, jnp.where(kind % 2 == 0, slot, -slot))
    runs = jnp.where(kind == 8, other[None, None, :], roster[None, None, :])
    match = jnp.where(kind % 4 < 2, (runs // 2 == expert // 2) & (kind < 8), False) | (runs == expert)
    best = jnp.max(jnp.where(match, value, -1000), axis=2)
    row = lax.broadcasted_iota(jnp.int32, shape[:2], 0)
    absent = jnp.where(row < 4, len(own), jnp.where(row < 8, len(par), NZ))
    return jnp.where(best == -1000, absent, jnp.abs(best))


def on_device(acts, grad_out, live_rows, placement, master, moment1, moment2):
    grad_in, gradient = step(placement, slot_table(placement), live_rows, acts, grad_out, master)
    new_master, new_moment1, new_moment2 = adam_update(master, moment1, moment2, gradient)
    return (grad_in, new_master, new_moment1, new_moment2)


def solution(mesh):
    in_specs = (
        P(("group", "dev"), None),
        P(("group", "dev"), None),
        P(("group", "dev")),
        P(),
        P("group", "dev", None),
        P("group", "dev", None),
        P("group", "dev", None),
    )
    out_specs = (
        P(("group", "dev"), None),
        P("group", "dev", None),
        P("group", "dev", None),
        P("group", "dev", None),
    )
    return jax.shard_map(
        on_device, mesh=mesh, in_specs=in_specs, out_specs=out_specs, check_vma=False
    )
```

```python
import functools

import jax
import jax.numpy as jnp
from jax import lax
from jax.experimental import pallas as pl
from jax.experimental.pallas import tpu as pltpu
from jax.sharding import PartitionSpec as P

beta_first = 0.9
beta_second = 0.95
learn_rate = 0.02
decay_rate = 0.1
epsilon = 1e-08
correct_first = 1.0 - (0.9**50) ** 2
correct_second = 1.0 - (0.95**50) ** 2

MESH = pl.DeviceIdType.MESH
NX, NY, NZ = 4, 8, 8


SKIP = 3
SPAN = 4
W_LOW = (-1, -2)
G_LOW = (-2, -1)


def offsets(low):
    return [(dx, dy) for dx in range(NX) for dy in range(low, low + SPAN)]


def by_distance(places):
    far = sorted(places, key=lambda d: (-(min(d[0], NX - d[0]) + abs(d[1])), d))
    return [d for d in far if d != (0, 0)]


def step_kernel(
    place_ref,
    place_vec,
    live_ref,
    acts_hbm,
    out_hbm,
    master_hbm,
    rows_ref,
    grad_ref,
    tab_vec,
    tab_ref,
    acts_ref,
    out_ref,
    master_ref,
    half_w,
    copy_g,
    weight,
    in_parts,
    w_own,
    w_par,
    w_send_own,
    w_send_par,
    g_own,
    g_par,
    d_send,
    d_own,
    d_par,
    r_send,
    r_recv,
    p_send,
    p_recv,
    pair_sem,
    ag_send_sem,
    ag_recv_sem,
    core_send_sem,
    core_recv_sem,
    gdev_send_sem,
    gdev_recv_sem,
    wdev_send_sem,
    wdev_recv_sem,
    d_sem,
    rs_send_sem,
    rs_recv_sem,
    local_sem,
):
    g = lax.axis_index("group")
    v = lax.axis_index("dev")
    z, c = g // 2, g % 2
    x, y = v // NY, v % NY
    w_places, g_places = [offsets(low) for low in W_LOW], [offsets(low) for low in G_LOW]
    slots = NX * SPAN
    vp = x * NY + lax.rem(y + SKIP, NY)
    members = NX * NY
    rows, width = half_w.shape[1:]
    w_all, d_recv = (w_own, w_par), (d_own, d_par)

    def at(dx, dy):
        return lax.rem(x + dx + NX, NX) * NY + lax.rem(y + dy + NY, NY)

    def held_by(vd):
        return (vd // NY) * NY + lax.rem(vd % NY + SKIP, NY)

    def zmod(k):
        return lax.rem(z + k + NZ, NZ)

    up_dev = (g, vp)
    down_dev = (g, x * NY + lax.rem(y + NY - SKIP, NY))
    core_dev = (z * 2 + 1 - c, v)
    z_dev = ((zmod(1) * 2 + c, v), (zmod(-1) * 2 + c, v))

    def remote(src, dst, ssem, rsem, dev):
        return pltpu.make_async_remote_copy(
            src_ref=src, dst_ref=dst, send_sem=ssem, recv_sem=rsem, device_id=dev, device_id_type=MESH
        )

    fetches = [
        pltpu.make_async_copy(src, dst, local_sem.at[3 + i])
        for i, (src, dst) in enumerate(((master_hbm, master_ref), (acts_hbm, acts_ref), (out_hbm, out_ref)))
    ]
    for cp in fetches:
        cp.start()
    barrier = pltpu.get_barrier_semaphore()
    near = sorted(set(w_places[0] + w_places[1] + g_places[0] + g_places[1]) - {(0, 0)})
    peers = [(g, at(dx, dy)) for dx, dy in near] + [up_dev, down_dev, core_dev]
    if NZ > 1:
        peers += list(z_dev)
    for dev in peers:
        pl.semaphore_signal(barrier, inc=1, device_id=dev, device_id_type=MESH)

    zero = jnp.zeros((rows, width), jnp.bfloat16)
    g_own[slots] = zero
    g_par[slots] = zero
    d_own[NZ] = zero
    d_par[NZ] = zero
    lanes = place_vec.shape[1]
    groups_per_row = lanes // members
    everyone = place_vec[pl.ds(g // groups_per_row, 1), :]
    shape = (4 * NZ, lanes)
    experts = lax.broadcasted_iota(jnp.int32, shape, 0)
    lane = lax.broadcasted_iota(jnp.int32, shape, 1)
    runs = jnp.broadcast_to(everyone, shape)
    place_of = lax.rem(g, groups_per_row) * members
    other_of = lax.rem(z * 2 + 1 - c, groups_per_row) * members
    in_group = (lane >= place_of) & (lane < place_of + members)
    in_other = (lane >= other_of) & (lane < other_of + members)
    source = lane & (members - 1)
    dx = (x - source // NY + NX) & (NX - 1)
    dy = ((y - (source & (NY - 1)) + NY // 2) & (NY - 1)) - NY // 2
    same_owner = in_group & ((runs >> 1) == (experts >> 1))
    same_expert = in_group & (runs == experts)
    column = lax.broadcasted_iota(jnp.int32, tab_vec.shape, 1)
    table = jnp.zeros(tab_vec.shape, jnp.int32)

    def put(table, k, match, value, absent):
        best = jnp.max(jnp.where(match, value, -1000), axis=1, keepdims=True)
        best = jnp.where(best == -1000, absent, jnp.abs(best))
        return jnp.where(column == k, best, table)

    for h in (0, 1):
        inside = (dy >= G_LOW[h]) & (dy < G_LOW[h] + SPAN)
        slot = jnp.where(inside, dx * SPAN + dy - G_LOW[h], slots)
        table = put(table, 4 * h, same_owner, slot, slots)
        table = put(table, 4 * h + 1, same_owner, -slot, slots)
        table = put(table, 4 * h + 2, same_expert, slot, slots)
        table = put(table, 4 * h + 3, same_expert, -slot, slots)
    table = put(table, 8, in_other & (runs == experts), experts >> 2, NZ)
    tab_vec[...] = table

    fetches[0].wait()
    half_w[...] = master_ref[...].astype(jnp.bfloat16)
    fetches[1].wait()
    fetches[2].wait()
    live = lax.broadcasted_iota(jnp.int32, acts_ref.shape, 0) < live_ref[0]
    masked = jnp.where(live, acts_ref[...], jnp.zeros((), jnp.bfloat16))
    strip = min(512, width)

    def copy_strip(i, carry):
        cols = pl.ds(pl.multiple_of(i * strip, strip), strip)
        product = lax.dot_general(
            masked, out_ref[:, cols], (((0,), (0,)), ((), ())), preferred_element_type=jnp.float32
        )
        copy_g[:, :, cols] = product.astype(jnp.bfloat16).reshape(members, rows, strip)
        return carry

    early_strips = width // strip // 2
    lax.fori_loop(0, early_strips, copy_strip, 0)
    pl.semaphore_wait(barrier, len(peers))

    sends = []

    def go(cp):
        cp.start()
        sends.append(cp)

    block = pl.ds(2 * g, 2)
    pair_copy = remote(half_w, w_all[1].at[block], pair_sem.at[0], pair_sem.at[1], down_dev)
    go(pair_copy)
    hops = ((NZ // 2, (NZ - 1) // 2), ((NZ - 1) // 2, NZ // 2))

    def ag(ring, way, step, src=None):
        k = step - 1
        o = zmod(-k if way == 0 else k) * 2 + c
        part = w_all[ring].at[pl.ds(2 * o, 2)]
        return remote(
            part if src is None else src,
            part,
            ag_send_sem.at[ring, way, k],
            ag_recv_sem.at[ring, way, k],
            z_dev[way],
        )

    def ag_arrived(ring, way, step):
        o = zmod(-step if way == 0 else step) * 2 + c
        part = w_all[ring].at[pl.ds(2 * o, 2)]
        remote(
            part, part, ag_send_sem.at[ring, way, step - 1], ag_recv_sem.at[ring, way, step - 1], z_dev[way]
        ).wait_recv()

    def core_copy(ring, k, src=None):
        o = zmod(-k) * 2 + c
        part = w_all[ring].at[pl.ds(2 * o, 2)]
        return remote(
            part if src is None else src,
            part,
            core_send_sem.at[ring, k],
            core_recv_sem.at[ring, k],
            core_dev,
        )

    def core_arrived(ring):
        for k in range(NZ):
            o = zmod(-k) * 2 + 1 - c
            part = w_all[ring].at[pl.ds(2 * o, 2)]
            remote(part, part, core_send_sem.at[ring, k], core_recv_sem.at[ring, k], core_dev).wait_recv()

    def launch(ring, src):
        for way in (0, 1):
            if hops[ring][way] > 0:
                go(ag(ring, way, 1, src))
        go(core_copy(ring, 0, src))

    def forward(ring, step):
        for way in (0, 1):
            if 1 <= step <= hops[ring][way]:
                ag_arrived(ring, way, step)
                if step < hops[ring][way]:
                    go(ag(ring, way, step + 1))
                go(core_copy(ring, step if way == 0 else NZ - step))

    launch(0, half_w)
    local_w = pltpu.make_async_copy(half_w, w_all[0].at[block], local_sem.at[0])
    local_w.start()
    table_copy = pltpu.make_async_copy(tab_vec, tab_ref, local_sem.at[6])
    table_copy.start()

    lax.fori_loop(early_strips, width // strip, copy_strip, 0)

    local_g = [
        pltpu.make_async_copy(copy_g.at[v], g_own.at[g_places[0].index((0, 0))], local_sem.at[1]),
        pltpu.make_async_copy(copy_g.at[vp], g_par.at[g_places[1].index((0, 0))], local_sem.at[2]),
    ]
    for cp in local_g:
        cp.start()
    g_waits = ([], [])

    def g_go(h, src, dst, s, dev):
        cp = remote(src, dst, gdev_send_sem.at[s], gdev_recv_sem.at[s], dev)
        go(cp)
        g_waits[h].append(cp)

    for dx, dy in by_distance(g_places[1]):
        vd = at(dx, dy)
        s = g_places[1].index((dx, dy))
        g_go(1, copy_g.at[held_by(vd)], g_par.at[s], slots + s, (g, vd))
    for dx, dy in by_distance(g_places[0]):
        vd = at(dx, dy)
        s = g_places[0].index((dx, dy))
        g_go(0, copy_g.at[vd], g_own.at[s], s, (g, vd))

    w_waits = {}

    def w_go(src, dst, s, dev, dx):
        cp = remote(src, dst, wdev_send_sem.at[s], wdev_recv_sem.at[s], dev)
        go(cp)
        w_waits.setdefault(dx, []).append(cp)

    w_send = (w_send_own, w_send_par)

    def deal(h):
        home = vp if h else v
        for dx, dy in by_distance(w_places[h]):
            vd = at(dx, dy)
            s = w_places[h].index((dx, dy))
            w_send[h][s] = w_all[h][place_ref[g * members + vd]]
            w_go(w_send[h].at[s], weight.at[home], h * slots + s, (g, vd), dx)
        weight[home] = w_all[h][place_ref[g * members + v]]

    recv = (g_own, g_par)

    def core_swap(h):
        return remote(d_send.at[h], d_recv[h].at[pl.ds(0, NZ)], d_sem.at[0, h], d_sem.at[1, h], core_dev)

    def give_core(h):
        local_g[h].wait()
        for cp in g_waits[h]:
            cp.wait_recv()

        def owner_sum(zz, carry):
            e = 2 * (2 * zz + 1 - c)
            first = recv[h][tab_ref[e, 4 * h]].astype(jnp.float32)
            second = recv[h][tab_ref[e, 4 * h + 1]].astype(jnp.float32)
            d_send[h, zz] = (first + second).astype(jnp.bfloat16)
            return carry

        lax.fori_loop(0, NZ, owner_sum, 0)
        go(core_swap(h))

    def chip_sum(h, zt, j):
        e = 2 * (2 * zt + c) + j
        first = recv[h][tab_ref[e, 4 * h + 2]].astype(jnp.float32)
        second = recv[h][tab_ref[e, 4 * h + 3]].astype(jnp.float32)
        return first + second + d_recv[h][tab_ref[e, 8]].astype(jnp.float32)

    def rs(h, way, step):
        return remote(
            r_send.at[h, way, step - 1],
            r_recv.at[h, way, step - 1],
            rs_send_sem.at[h, way, step - 1],
            rs_recv_sem.at[h, way, step - 1],
            z_dev[1 - way],
        )

    def rs_step(h, step):
        for way in (0, 1):
            length = hops[h][way]
            if step > length:
                continue
            away = length - step + 1
            zt = zmod(-away if way == 0 else away)
            if step > 1:
                rs(h, way, step - 1).wait_recv()
            for j in (0, 1):
                total = chip_sum(h, zt, j)
                if step > 1:
                    total = total + r_recv[h, way, step - 2, j].astype(jnp.float32)
                r_send[h, way, step - 1, j] = total.astype(jnp.bfloat16)
            go(rs(h, way, step))

    def rs_last(h):
        for way in (0, 1):
            if hops[h][way] > 0:
                rs(h, way, hops[h][way]).wait_recv()

    def home_sum(h, j):
        total = chip_sum(h, z, j)
        for way in (0, 1):
            if hops[h][way] > 0:
                total = total + r_recv[h, way, hops[h][way] - 1, j].astype(jnp.float32)
        return total

    steps = NZ // 2
    forward(0, 1)
    forward(0, 2)
    pair_copy.wait_recv()
    launch(1, None)
    forward(0, 3)
    forward(1, 1)
    table_copy.wait()
    give_core(1)
    for k in range(4, steps + 1):
        forward(0, k)
    forward(1, 2)
    core_swap(1).wait_recv()
    rs_step(1, 1)
    local_w.wait()
    core_arrived(0)
    deal(0)
    forward(1, 3)
    rs_step(1, 2)
    for k in range(4, steps + 1):
        forward(1, k)
    core_arrived(1)
    deal(1)
    rs_step(1, 3)
    give_core(0)
    core_swap(0).wait_recv()
    rs_step(0, 1)
    for step in range(4, steps + 1):
        rs_step(1, step)
    rs_last(1)
    for j in (0, 1):
        p_send[j] = home_sum(1, j).astype(jnp.bfloat16)
    back = remote(p_send, p_recv, pair_sem.at[2], pair_sem.at[3], up_dev)
    go(back)
    for step in range(2, steps + 1):
        rs_step(0, step)
    rs_last(0)

    kept = lax.broadcasted_iota(jnp.int32, (acts_ref.shape[0], NY * rows), 0) < live_ref[0]
    for i, dx in enumerate(sorted(range(NX), key=lambda d: (min(d, NX - d), d))):
        if i == NX - 1:
            back.wait_recv()
            for j in (0, 1):
                grad_ref[j] = home_sum(0, j) + p_recv[j].astype(jnp.float32)
        for cp in w_waits.get(dx, []):
            cp.wait_recv()
        xs = lax.rem(x - dx + NX, NX)
        part = weight[pl.ds(xs * NY, NY)].reshape(NY * rows, width)
        product = lax.dot_general(
            out_ref[...], part, (((1,), (1,)), ((), ())), preferred_element_type=jnp.float32
        )
        in_parts[xs] = jnp.where(kept, product, jnp.zeros((), jnp.float32)).astype(jnp.bfloat16)
    for xs in range(NX):
        rows_ref[:, xs * NY * rows : (xs + 1) * NY * rows] = in_parts[xs]
    for cp in sends:
        cp.wait_send()


def step(placement, live_rows, acts, grad_out, master):
    rows, width = master.shape[1:]
    slots = NX * SPAN
    lanes = min(128, placement.shape[0])
    owners = 2 * NZ
    steps = max(1, NZ // 2)
    dma = pltpu.SemaphoreType.DMA
    vmem = pl.BlockSpec(memory_space=pltpu.VMEM)
    smem = pl.BlockSpec(memory_space=pltpu.SMEM)
    anywhere = pl.BlockSpec(memory_space=pl.ANY)

    def blocks(*lead):
        return pltpu.VMEM(lead + (rows, width), jnp.bfloat16)

    return pl.pallas_call(
        step_kernel,
        name="step",
        out_shape=(
            jax.ShapeDtypeStruct(acts.shape, jnp.bfloat16),
            jax.ShapeDtypeStruct(master.shape, jnp.float32),
        ),
        in_specs=[smem, vmem, smem, anywhere, anywhere, anywhere],
        out_specs=(vmem, vmem),
        scratch_shapes=[
            pltpu.VMEM((2 * owners, 128), jnp.int32),
            pltpu.SMEM((2 * owners, 128), jnp.int32),
            pltpu.VMEM(acts.shape, acts.dtype),
            pltpu.VMEM(grad_out.shape, grad_out.dtype),
            pltpu.VMEM(master.shape, master.dtype),
            blocks(2),
            blocks(NX * NY),
            blocks(NX * NY),
            pltpu.VMEM((NX, acts.shape[0], NY * rows), jnp.bfloat16),
            blocks(2 * owners),
            blocks(2 * owners),
            blocks(slots),
            blocks(slots),
            blocks(slots + 1),
            blocks(slots + 1),
            blocks(2, NZ),
            blocks(NZ + 1),
            blocks(NZ + 1),
            blocks(2, 2, steps, 2),
            blocks(2, 2, steps, 2),
            blocks(2),
            blocks(2),
            dma((4,)),
            dma((2, 2, steps)),
            dma((2, 2, steps)),
            dma((2, NZ)),
            dma((2, NZ)),
            dma((2 * slots,)),
            dma((2 * slots,)),
            dma((2 * slots,)),
            dma((2 * slots,)),
            dma((2, 2)),
            dma((2, 2, steps)),
            dma((2, 2, steps)),
            dma((7,)),
        ],
        compiler_params=pltpu.CompilerParams(
            collective_id=0, has_side_effects=True, vmem_limit_bytes=60 * 2**20
        ),
    )(placement, placement.reshape(-1, lanes), live_rows, acts, grad_out, master)


def adam_update(master, moment1, moment2, gradient):
    new_moment1 = beta_first * moment1 + (1.0 - beta_first) * gradient
    new_moment2 = beta_second * moment2 + (1.0 - beta_second) * gradient * gradient
    root = jnp.sqrt(new_moment2 * (correct_first**2 / correct_second))
    ascent = new_moment1 / (root + correct_first * epsilon)
    new_master = master - learn_rate * (ascent + decay_rate * master)
    return (new_master, new_moment1, new_moment2)


def on_device(acts, grad_out, live_rows, placement, master, moment1, moment2):
    grad_in, gradient = step(placement, live_rows, acts, grad_out, master)
    new_master, new_moment1, new_moment2 = adam_update(master, moment1, moment2, gradient)
    return (grad_in, new_master, new_moment1, new_moment2)


def solution(mesh):
    in_specs = (
        P(("group", "dev"), None),
        P(("group", "dev"), None),
        P(("group", "dev")),
        P(),
        P("group", "dev", None),
        P("group", "dev", None),
        P("group", "dev", None),
    )
    out_specs = (
        P(("group", "dev"), None),
        P("group", "dev", None),
        P("group", "dev", None),
        P("group", "dev", None),
    )
    return jax.shard_map(
        on_device, mesh=mesh, in_specs=in_specs, out_specs=out_specs, check_vma=False
    )
```

```python
import functools

import jax
import jax.numpy as jnp
from jax import lax
from jax.experimental import pallas as pl
from jax.experimental.pallas import tpu as pltpu
from jax.sharding import PartitionSpec as P

beta_first = 0.9
beta_second = 0.95
learn_rate = 0.02
decay_rate = 0.1
epsilon = 1e-08
correct_first = 1.0 - (0.9**50) ** 2
correct_second = 1.0 - (0.95**50) ** 2

MESH = pl.DeviceIdType.MESH
NX, NY, NZ = 4, 8, 8


SKIP = 3
SPAN = 4
W_LOW = (-1, -2)
G_LOW = (-2, -1)


def offsets(low):
    return [(dx, dy) for dx in range(NX) for dy in range(low, low + SPAN)]


def by_distance(places):
    far = sorted(places, key=lambda d: (-min(d[0], NX - d[0]), abs(d[1]), d[1], d[0]))
    return [d for d in far if d != (0, 0)]


def step_kernel(
    place_ref,
    place_vec,
    live_ref,
    acts_hbm,
    out_hbm,
    master_hbm,
    rows_ref,
    grad_ref,
    tab_vec,
    tab_ref,
    acts_ref,
    out_ref,
    master_ref,
    half_w,
    copy_g,
    weight,
    in_parts,
    w_own,
    w_par,
    w_send_own,
    w_send_par,
    g_own,
    g_par,
    d_send,
    d_own,
    d_par,
    r_send,
    r_recv,
    p_send,
    p_recv,
    pair_sem,
    ag_send_sem,
    ag_recv_sem,
    core_send_sem,
    core_recv_sem,
    gdev_send_sem,
    gdev_recv_sem,
    wdev_send_sem,
    wdev_recv_sem,
    d_sem,
    rs_send_sem,
    rs_recv_sem,
    local_sem,
):
    g = lax.axis_index("group")
    v = lax.axis_index("dev")
    z, c = g // 2, g % 2
    x, y = v // NY, v % NY
    w_places, g_places = [offsets(low) for low in W_LOW], [offsets(low) for low in G_LOW]
    slots = NX * SPAN
    vp = x * NY + lax.rem(y + SKIP, NY)
    members = NX * NY
    rows, width = half_w.shape[1:]
    w_all, d_recv = (w_own, w_par), (d_own, d_par)

    def at(dx, dy):
        return lax.rem(x + dx + NX, NX) * NY + lax.rem(y + dy + NY, NY)

    def held_by(vd):
        return (vd // NY) * NY + lax.rem(vd % NY + SKIP, NY)

    def zmod(k):
        return lax.rem(z + k + NZ, NZ)

    up_dev = (g, vp)
    down_dev = (g, x * NY + lax.rem(y + NY - SKIP, NY))
    core_dev = (z * 2 + 1 - c, v)
    z_dev = ((zmod(1) * 2 + c, v), (zmod(-1) * 2 + c, v))

    def remote(src, dst, ssem, rsem, dev):
        return pltpu.make_async_remote_copy(
            src_ref=src, dst_ref=dst, send_sem=ssem, recv_sem=rsem, device_id=dev, device_id_type=MESH
        )

    fetches = [
        pltpu.make_async_copy(src, dst, local_sem.at[3 + i])
        for i, (src, dst) in enumerate(((master_hbm, master_ref), (acts_hbm, acts_ref), (out_hbm, out_ref)))
    ]
    for cp in fetches:
        cp.start()
    barrier = pltpu.get_barrier_semaphore()
    near = sorted(set(w_places[0] + w_places[1] + g_places[0] + g_places[1]) - {(0, 0)})
    peers = [(g, at(dx, dy)) for dx, dy in near] + [up_dev, down_dev, core_dev]
    if NZ > 1:
        peers += list(z_dev)
    for dev in peers:
        pl.semaphore_signal(barrier, inc=1, device_id=dev, device_id_type=MESH)

    zero = jnp.zeros((rows, width), jnp.bfloat16)
    g_own[slots] = zero
    g_par[slots] = zero
    d_own[NZ] = zero
    d_par[NZ] = zero
    lanes = place_vec.shape[1]
    groups_per_row = lanes // members
    everyone = place_vec[pl.ds(g // groups_per_row, 1), :]
    shape = (4 * NZ, lanes)
    experts = lax.broadcasted_iota(jnp.int32, shape, 0)
    lane = lax.broadcasted_iota(jnp.int32, shape, 1)
    runs = jnp.broadcast_to(everyone, shape)
    place_of = lax.rem(g, groups_per_row) * members
    other_of = lax.rem(z * 2 + 1 - c, groups_per_row) * members
    in_group = (lane >= place_of) & (lane < place_of + members)
    in_other = (lane >= other_of) & (lane < other_of + members)
    source = lane & (members - 1)
    dx = (x - source // NY + NX) & (NX - 1)
    dy = ((y - (source & (NY - 1)) + NY // 2) & (NY - 1)) - NY // 2
    same_owner = in_group & ((runs >> 1) == (experts >> 1))
    same_expert = in_group & (runs == experts)
    column = lax.broadcasted_iota(jnp.int32, tab_vec.shape, 1)
    table = jnp.zeros(tab_vec.shape, jnp.int32)

    def put(table, k, match, value, absent):
        best = jnp.max(jnp.where(match, value, -1000), axis=1, keepdims=True)
        best = jnp.where(best == -1000, absent, jnp.abs(best))
        return jnp.where(column == k, best, table)

    for h in (0, 1):
        inside = (dy >= G_LOW[h]) & (dy < G_LOW[h] + SPAN)
        slot = jnp.where(inside, dx * SPAN + dy - G_LOW[h], slots)
        table = put(table, 4 * h, same_owner, slot, slots)
        table = put(table, 4 * h + 1, same_owner, -slot, slots)
        table = put(table, 4 * h + 2, same_expert, slot, slots)
        table = put(table, 4 * h + 3, same_expert, -slot, slots)
    table = put(table, 8, in_other & (runs == experts), experts >> 2, NZ)
    tab_vec[...] = table

    fetches[0].wait()
    half_w[...] = master_ref[...].astype(jnp.bfloat16)
    fetches[1].wait()
    fetches[2].wait()
    live = lax.broadcasted_iota(jnp.int32, acts_ref.shape, 0) < live_ref[0]
    masked = jnp.where(live, acts_ref[...], jnp.zeros((), jnp.bfloat16))
    strip = min(512, width)

    def copy_strip(i, carry):
        cols = pl.ds(pl.multiple_of(i * strip, strip), strip)
        product = lax.dot_general(
            masked, out_ref[:, cols], (((0,), (0,)), ((), ())), preferred_element_type=jnp.float32
        )
        copy_g[:, :, cols] = product.astype(jnp.bfloat16).reshape(members, rows, strip)
        return carry

    early_strips = width // strip // 2
    lax.fori_loop(0, early_strips, copy_strip, 0)
    pl.semaphore_wait(barrier, len(peers))

    sends = []

    def go(cp):
        cp.start()
        sends.append(cp)

    block = pl.ds(2 * g, 2)
    pair_copy = remote(half_w, w_all[1].at[block], pair_sem.at[0], pair_sem.at[1], down_dev)
    go(pair_copy)
    hops = ((NZ // 2, (NZ - 1) // 2), ((NZ - 1) // 2, NZ // 2))

    def ag(ring, way, step, j, src=None):
        k = step - 1
        o = zmod(-k if way == 0 else k) * 2 + c
        part = w_all[ring].at[2 * o + j]
        return remote(
            part if src is None else src.at[j],
            part,
            ag_send_sem.at[ring, way, k, j],
            ag_recv_sem.at[ring, way, k, j],
            z_dev[way],
        )

    def ag_arrived(ring, way, step, j):
        o = zmod(-step if way == 0 else step) * 2 + c
        part = w_all[ring].at[2 * o + j]
        k = step - 1
        remote(
            part, part, ag_send_sem.at[ring, way, k, j], ag_recv_sem.at[ring, way, k, j], z_dev[way]
        ).wait_recv()

    def core_copy(ring, k, src=None):
        o = zmod(-k) * 2 + c
        part = w_all[ring].at[pl.ds(2 * o, 2)]
        return remote(
            part if src is None else src,
            part,
            core_send_sem.at[ring, k],
            core_recv_sem.at[ring, k],
            core_dev,
        )

    def core_arrived(ring):
        for k in range(NZ):
            o = zmod(-k) * 2 + 1 - c
            part = w_all[ring].at[pl.ds(2 * o, 2)]
            remote(part, part, core_send_sem.at[ring, k], core_recv_sem.at[ring, k], core_dev).wait_recv()

    def launch(ring, src):
        for j in (0, 1):
            for way in (0, 1):
                if hops[ring][way] > 0:
                    go(ag(ring, way, 1, j, src))
        go(core_copy(ring, 0, src))

    def forward(ring, step):
        ways = [way for way in (0, 1) if 1 <= step <= hops[ring][way]]
        for j in (0, 1):
            for way in ways:
                ag_arrived(ring, way, step, j)
                if step < hops[ring][way]:
                    go(ag(ring, way, step + 1, j))
        for way in ways:
            go(core_copy(ring, step if way == 0 else NZ - step))

    launch(0, half_w)
    local_w = pltpu.make_async_copy(half_w, w_all[0].at[block], local_sem.at[0])
    local_w.start()
    table_copy = pltpu.make_async_copy(tab_vec, tab_ref, local_sem.at[6])
    table_copy.start()

    lax.fori_loop(early_strips, width // strip, copy_strip, 0)

    local_g = [
        pltpu.make_async_copy(copy_g.at[v], g_own.at[g_places[0].index((0, 0))], local_sem.at[1]),
        pltpu.make_async_copy(copy_g.at[vp], g_par.at[g_places[1].index((0, 0))], local_sem.at[2]),
    ]
    for cp in local_g:
        cp.start()
    g_waits = ([], [])

    def g_go(h, src, dst, s, dev):
        cp = remote(src, dst, gdev_send_sem.at[s], gdev_recv_sem.at[s], dev)
        go(cp)
        g_waits[h].append(cp)

    for dx, dy in by_distance(g_places[1]):
        vd = at(dx, dy)
        s = g_places[1].index((dx, dy))
        g_go(1, copy_g.at[held_by(vd)], g_par.at[s], slots + s, (g, vd))
    for dx, dy in by_distance(g_places[0]):
        vd = at(dx, dy)
        s = g_places[0].index((dx, dy))
        g_go(0, copy_g.at[vd], g_own.at[s], s, (g, vd))

    w_waits = {}

    def w_go(src, dst, s, dev, dx):
        cp = remote(src, dst, wdev_send_sem.at[s], wdev_recv_sem.at[s], dev)
        go(cp)
        w_waits.setdefault(dx, []).append(cp)

    w_send = (w_send_own, w_send_par)

    def deal(h):
        home = vp if h else v
        for dx, dy in by_distance(w_places[h]):
            vd = at(dx, dy)
            s = w_places[h].index((dx, dy))
            w_send[h][s] = w_all[h][place_ref[g * members + vd]]
            w_go(w_send[h].at[s], weight.at[home], h * slots + s, (g, vd), dx)
        weight[home] = w_all[h][place_ref[g * members + v]]

    recv = (g_own, g_par)

    def core_swap(h):
        return remote(d_send.at[h], d_recv[h].at[pl.ds(0, NZ)], d_sem.at[0, h], d_sem.at[1, h], core_dev)

    def give_core(h):
        local_g[h].wait()
        for cp in g_waits[h]:
            cp.wait_recv()

        def owner_sum(zz, carry):
            e = 2 * (2 * zz + 1 - c)
            first = recv[h][tab_ref[e, 4 * h]].astype(jnp.float32)
            second = recv[h][tab_ref[e, 4 * h + 1]].astype(jnp.float32)
            d_send[h, zz] = (first + second).astype(jnp.bfloat16)
            return carry

        lax.fori_loop(0, NZ, owner_sum, 0)
        go(core_swap(h))

    def chip_sum(h, zt, j):
        e = 2 * (2 * zt + c) + j
        first = recv[h][tab_ref[e, 4 * h + 2]].astype(jnp.float32)
        second = recv[h][tab_ref[e, 4 * h + 3]].astype(jnp.float32)
        return first + second + d_recv[h][tab_ref[e, 8]].astype(jnp.float32)

    def rs(h, way, step, j):
        return remote(
            r_send.at[h, way, step - 1, j],
            r_recv.at[h, way, step - 1, j],
            rs_send_sem.at[h, way, step - 1, j],
            rs_recv_sem.at[h, way, step - 1, j],
            z_dev[1 - way],
        )

    def rs_step(h, step):
        for j in (0, 1):
            for way in (0, 1):
                length = hops[h][way]
                if step > length:
                    continue
                away = length - step + 1
                zt = zmod(-away if way == 0 else away)
                if step > 1:
                    rs(h, way, step - 1, j).wait_recv()
                total = chip_sum(h, zt, j)
                if step > 1:
                    total = total + r_recv[h, way, step - 2, j].astype(jnp.float32)
                r_send[h, way, step - 1, j] = total.astype(jnp.bfloat16)
                go(rs(h, way, step, j))

    def rs_last(h):
        for j in (0, 1):
            for way in (0, 1):
                if hops[h][way] > 0:
                    rs(h, way, hops[h][way], j).wait_recv()

    def home_sum(h, j):
        total = chip_sum(h, z, j)
        for way in (0, 1):
            if hops[h][way] > 0:
                total = total + r_recv[h, way, hops[h][way] - 1, j].astype(jnp.float32)
        return total

    steps = NZ // 2
    forward(0, 1)
    forward(0, 2)
    pair_copy.wait_recv()
    launch(1, None)
    forward(0, 3)
    forward(1, 1)
    table_copy.wait()
    give_core(1)
    for k in range(4, steps + 1):
        forward(0, k)
    forward(1, 2)
    core_swap(1).wait_recv()
    rs_step(1, 1)
    local_w.wait()
    core_arrived(0)
    deal(0)
    forward(1, 3)
    rs_step(1, 2)
    for k in range(4, steps + 1):
        forward(1, k)
    core_arrived(1)
    deal(1)
    rs_step(1, 3)
    give_core(0)
    core_swap(0).wait_recv()
    rs_step(0, 1)
    for step in range(4, steps + 1):
        rs_step(1, step)
    if steps > 1:
        rs_step(0, 2)
    rs_last(1)
    for j in (0, 1):
        p_send[j] = home_sum(1, j).astype(jnp.bfloat16)
    back = remote(p_send, p_recv, pair_sem.at[2], pair_sem.at[3], up_dev)
    go(back)
    for step in range(3, steps + 1):
        rs_step(0, step)

    kept = lax.broadcasted_iota(jnp.int32, (acts_ref.shape[0], NY * rows), 0) < live_ref[0]
    for i, dx in enumerate(sorted(range(NX), key=lambda d: (-min(d, NX - d), d))):
        if i == NX - 1:
            rs_last(0)
            back.wait_recv()
            for j in (0, 1):
                grad_ref[j] = home_sum(0, j) + p_recv[j].astype(jnp.float32)
        for cp in w_waits.get(dx, []):
            cp.wait_recv()
        xs = lax.rem(x - dx + NX, NX)
        part = weight[pl.ds(xs * NY, NY)].reshape(NY * rows, width)
        product = lax.dot_general(
            out_ref[...], part, (((1,), (1,)), ((), ())), preferred_element_type=jnp.float32
        )
        in_parts[xs] = jnp.where(kept, product, jnp.zeros((), jnp.float32)).astype(jnp.bfloat16)
    for xs in range(NX):
        rows_ref[:, xs * NY * rows : (xs + 1) * NY * rows] = in_parts[xs]
    for cp in sends:
        cp.wait_send()


def step(placement, live_rows, acts, grad_out, master):
    rows, width = master.shape[1:]
    slots = NX * SPAN
    lanes = min(128, placement.shape[0])
    owners = 2 * NZ
    steps = max(1, NZ // 2)
    dma = pltpu.SemaphoreType.DMA
    vmem = pl.BlockSpec(memory_space=pltpu.VMEM)
    smem = pl.BlockSpec(memory_space=pltpu.SMEM)
    anywhere = pl.BlockSpec(memory_space=pl.ANY)

    def blocks(*lead):
        return pltpu.VMEM(lead + (rows, width), jnp.bfloat16)

    return pl.pallas_call(
        step_kernel,
        name="step",
        out_shape=(
            jax.ShapeDtypeStruct(acts.shape, jnp.bfloat16),
            jax.ShapeDtypeStruct(master.shape, jnp.float32),
        ),
        in_specs=[smem, vmem, smem, anywhere, anywhere, anywhere],
        out_specs=(vmem, vmem),
        scratch_shapes=[
            pltpu.VMEM((2 * owners, 128), jnp.int32),
            pltpu.SMEM((2 * owners, 128), jnp.int32),
            pltpu.VMEM(acts.shape, acts.dtype),
            pltpu.VMEM(grad_out.shape, grad_out.dtype),
            pltpu.VMEM(master.shape, master.dtype),
            blocks(2),
            blocks(NX * NY),
            blocks(NX * NY),
            pltpu.VMEM((NX, acts.shape[0], NY * rows), jnp.bfloat16),
            blocks(2 * owners),
            blocks(2 * owners),
            blocks(slots),
            blocks(slots),
            blocks(slots + 1),
            blocks(slots + 1),
            blocks(2, NZ),
            blocks(NZ + 1),
            blocks(NZ + 1),
            blocks(2, 2, steps, 2),
            blocks(2, 2, steps, 2),
            blocks(2),
            blocks(2),
            dma((4,)),
            dma((2, 2, steps, 2)),
            dma((2, 2, steps, 2)),
            dma((2, NZ)),
            dma((2, NZ)),
            dma((2 * slots,)),
            dma((2 * slots,)),
            dma((2 * slots,)),
            dma((2 * slots,)),
            dma((2, 2)),
            dma((2, 2, steps, 2)),
            dma((2, 2, steps, 2)),
            dma((7,)),
        ],
        compiler_params=pltpu.CompilerParams(
            collective_id=0, has_side_effects=True, vmem_limit_bytes=60 * 2**20
        ),
    )(placement, placement.reshape(-1, lanes), live_rows, acts, grad_out, master)


def adam_update(master, moment1, moment2, gradient):
    new_moment1 = beta_first * moment1 + (1.0 - beta_first) * gradient
    new_moment2 = beta_second * moment2 + (1.0 - beta_second) * gradient * gradient
    root = jnp.sqrt(new_moment2 * (correct_first**2 / correct_second))
    ascent = new_moment1 / (root + correct_first * epsilon)
    new_master = master - learn_rate * (ascent + decay_rate * master)
    return (new_master, new_moment1, new_moment2)


def on_device(acts, grad_out, live_rows, placement, master, moment1, moment2):
    grad_in, gradient = step(placement, live_rows, acts, grad_out, master)
    new_master, new_moment1, new_moment2 = adam_update(master, moment1, moment2, gradient)
    return (grad_in, new_master, new_moment1, new_moment2)


def solution(mesh):
    in_specs = (
        P(("group", "dev"), None),
        P(("group", "dev"), None),
        P(("group", "dev")),
        P(),
        P("group", "dev", None),
        P("group", "dev", None),
        P("group", "dev", None),
    )
    out_specs = (
        P(("group", "dev"), None),
        P("group", "dev", None),
        P("group", "dev", None),
        P("group", "dev", None),
    )
    return jax.shard_map(
        on_device, mesh=mesh, in_specs=in_specs, out_specs=out_specs, check_vma=False
    )
```

```python
import functools

import jax
import jax.numpy as jnp
from jax import lax
from jax.experimental import pallas as pl
from jax.experimental.pallas import tpu as pltpu
from jax.sharding import PartitionSpec as P

beta_first = 0.9
beta_second = 0.95
learn_rate = 0.02
decay_rate = 0.1
epsilon = 1e-08
correct_first = 1.0 - (0.9**50) ** 2
correct_second = 1.0 - (0.95**50) ** 2

MESH = pl.DeviceIdType.MESH
NX, NY, NZ = 4, 8, 8


SKIP = 3
SPAN = 4
W_LOW = (-1, -2)
G_LOW = (-2, -1)


def offsets(low):
    return [(dx, dy) for dx in range(NX) for dy in range(low, low + SPAN)]


def by_distance(places):
    far = sorted(places, key=lambda d: (min(d[0], NX - d[0]), abs(d[1]), d[1], d[0]))
    return [d for d in far if d != (0, 0)]


def step_kernel(
    place_ref,
    place_vec,
    live_ref,
    acts_hbm,
    out_hbm,
    master_hbm,
    rows_ref,
    grad_ref,
    tab_vec,
    tab_ref,
    acts_ref,
    out_ref,
    master_ref,
    half_w,
    copy_g,
    weight,
    in_parts,
    w_own,
    w_par,
    w_send_own,
    w_send_par,
    g_own,
    g_par,
    d_send,
    d_own,
    d_par,
    r_send,
    r_recv,
    p_send,
    p_recv,
    pair_sem,
    ag_send_sem,
    ag_recv_sem,
    core_send_sem,
    core_recv_sem,
    gdev_send_sem,
    gdev_recv_sem,
    wdev_send_sem,
    wdev_recv_sem,
    d_sem,
    rs_send_sem,
    rs_recv_sem,
    local_sem,
):
    g = lax.axis_index("group")
    v = lax.axis_index("dev")
    z, c = g // 2, g % 2
    x, y = v // NY, v % NY
    w_places, g_places = [offsets(low) for low in W_LOW], [offsets(low) for low in G_LOW]
    slots = NX * SPAN
    vp = x * NY + lax.rem(y + SKIP, NY)
    members = NX * NY
    rows, width = half_w.shape[1:]
    w_all, d_recv = (w_own, w_par), (d_own, d_par)

    def at(dx, dy):
        return lax.rem(x + dx + NX, NX) * NY + lax.rem(y + dy + NY, NY)

    def held_by(vd):
        return (vd // NY) * NY + lax.rem(vd % NY + SKIP, NY)

    def zmod(k):
        return lax.rem(z + k + NZ, NZ)

    up_dev = (g, vp)
    down_dev = (g, x * NY + lax.rem(y + NY - SKIP, NY))
    core_dev = (z * 2 + 1 - c, v)
    z_dev = ((zmod(1) * 2 + c, v), (zmod(-1) * 2 + c, v))

    def remote(src, dst, ssem, rsem, dev):
        return pltpu.make_async_remote_copy(
            src_ref=src, dst_ref=dst, send_sem=ssem, recv_sem=rsem, device_id=dev, device_id_type=MESH
        )

    fetches = [
        pltpu.make_async_copy(src, dst, local_sem.at[3 + i])
        for i, (src, dst) in enumerate(((master_hbm, master_ref), (acts_hbm, acts_ref), (out_hbm, out_ref)))
    ]
    for cp in fetches:
        cp.start()
    barrier = pltpu.get_barrier_semaphore()
    near = sorted(set(w_places[0] + w_places[1] + g_places[0] + g_places[1]) - {(0, 0)})
    peers = [(g, at(dx, dy)) for dx, dy in near] + [up_dev, down_dev, core_dev]
    if NZ > 1:
        peers += list(z_dev)
    for dev in peers:
        pl.semaphore_signal(barrier, inc=1, device_id=dev, device_id_type=MESH)

    zero = jnp.zeros((rows, width), jnp.bfloat16)
    g_own[slots] = zero
    g_par[slots] = zero
    d_own[NZ] = zero
    d_par[NZ] = zero
    lanes = place_vec.shape[1]
    groups_per_row = lanes // members
    everyone = place_vec[pl.ds(g // groups_per_row, 1), :]
    shape = (4 * NZ, lanes)
    experts = lax.broadcasted_iota(jnp.int32, shape, 0)
    lane = lax.broadcasted_iota(jnp.int32, shape, 1)
    runs = jnp.broadcast_to(everyone, shape)
    place_of = lax.rem(g, groups_per_row) * members
    other_of = lax.rem(z * 2 + 1 - c, groups_per_row) * members
    in_group = (lane >= place_of) & (lane < place_of + members)
    in_other = (lane >= other_of) & (lane < other_of + members)
    source = lane & (members - 1)
    dx = (x - source // NY + NX) & (NX - 1)
    dy = ((y - (source & (NY - 1)) + NY // 2) & (NY - 1)) - NY // 2
    same_owner = in_group & ((runs >> 1) == (experts >> 1))
    same_expert = in_group & (runs == experts)
    column = lax.broadcasted_iota(jnp.int32, tab_vec.shape, 1)
    table = jnp.zeros(tab_vec.shape, jnp.int32)

    def put(table, k, match, value, absent):
        best = jnp.max(jnp.where(match, value, -1000), axis=1, keepdims=True)
        best = jnp.where(best == -1000, absent, jnp.abs(best))
        return jnp.where(column == k, best, table)

    for h in (0, 1):
        inside = (dy >= G_LOW[h]) & (dy < G_LOW[h] + SPAN)
        slot = jnp.where(inside, dx * SPAN + dy - G_LOW[h], slots)
        table = put(table, 4 * h, same_owner, slot, slots)
        table = put(table, 4 * h + 1, same_owner, -slot, slots)
        table = put(table, 4 * h + 2, same_expert, slot, slots)
        table = put(table, 4 * h + 3, same_expert, -slot, slots)
    table = put(table, 8, in_other & (runs == experts), experts >> 2, NZ)
    tab_vec[...] = table

    fetches[0].wait()
    half_w[...] = master_ref[...].astype(jnp.bfloat16)
    fetches[1].wait()
    fetches[2].wait()
    live = lax.broadcasted_iota(jnp.int32, acts_ref.shape, 0) < live_ref[0]
    masked = jnp.where(live, acts_ref[...], jnp.zeros((), jnp.bfloat16))
    strip = min(512, width)

    def copy_strip(i, carry):
        cols = pl.ds(pl.multiple_of(i * strip, strip), strip)
        product = lax.dot_general(
            masked, out_ref[:, cols], (((0,), (0,)), ((), ())), preferred_element_type=jnp.float32
        )
        copy_g[:, :, cols] = product.astype(jnp.bfloat16).reshape(members, rows, strip)
        return carry

    early_strips = width // strip // 2
    lax.fori_loop(0, early_strips, copy_strip, 0)
    pl.semaphore_wait(barrier, len(peers))

    sends = []

    def go(cp):
        cp.start()
        sends.append(cp)

    block = pl.ds(2 * g, 2)
    pair_copy = remote(half_w, w_all[1].at[block], pair_sem.at[0], pair_sem.at[1], down_dev)
    go(pair_copy)
    hops = ((NZ // 2, (NZ - 1) // 2), ((NZ - 1) // 2, NZ // 2))

    def ag(ring, way, step, j, src=None):
        k = step - 1
        o = zmod(-k if way == 0 else k) * 2 + c
        part = w_all[ring].at[2 * o + j]
        return remote(
            part if src is None else src.at[j],
            part,
            ag_send_sem.at[ring, way, k, j],
            ag_recv_sem.at[ring, way, k, j],
            z_dev[way],
        )

    def ag_arrived(ring, way, step, j):
        o = zmod(-step if way == 0 else step) * 2 + c
        part = w_all[ring].at[2 * o + j]
        k = step - 1
        remote(
            part, part, ag_send_sem.at[ring, way, k, j], ag_recv_sem.at[ring, way, k, j], z_dev[way]
        ).wait_recv()

    def core_copy(ring, k, src=None):
        o = zmod(-k) * 2 + c
        part = w_all[ring].at[pl.ds(2 * o, 2)]
        return remote(
            part if src is None else src,
            part,
            core_send_sem.at[ring, k],
            core_recv_sem.at[ring, k],
            core_dev,
        )

    def core_arrived(ring):
        for k in range(NZ):
            o = zmod(-k) * 2 + 1 - c
            part = w_all[ring].at[pl.ds(2 * o, 2)]
            remote(part, part, core_send_sem.at[ring, k], core_recv_sem.at[ring, k], core_dev).wait_recv()

    def launch(ring, src):
        for j in (0, 1):
            for way in (0, 1):
                if hops[ring][way] > 0:
                    go(ag(ring, way, 1, j, src))
        go(core_copy(ring, 0, src))

    def forward(ring, step):
        ways = [way for way in (0, 1) if 1 <= step <= hops[ring][way]]
        for j in (0, 1):
            for way in ways:
                ag_arrived(ring, way, step, j)
                if step < hops[ring][way]:
                    go(ag(ring, way, step + 1, j))
        for way in ways:
            go(core_copy(ring, step if way == 0 else NZ - step))

    launch(0, half_w)
    local_w = pltpu.make_async_copy(half_w, w_all[0].at[block], local_sem.at[0])
    local_w.start()
    table_copy = pltpu.make_async_copy(tab_vec, tab_ref, local_sem.at[6])
    table_copy.start()

    lax.fori_loop(early_strips, width // strip, copy_strip, 0)

    local_g = [
        pltpu.make_async_copy(copy_g.at[v], g_own.at[g_places[0].index((0, 0))], local_sem.at[1]),
        pltpu.make_async_copy(copy_g.at[vp], g_par.at[g_places[1].index((0, 0))], local_sem.at[2]),
    ]
    for cp in local_g:
        cp.start()
    g_waits = ([], [])

    def g_go(h, src, dst, s, dev):
        cp = remote(src, dst, gdev_send_sem.at[s], gdev_recv_sem.at[s], dev)
        go(cp)
        g_waits[h].append(cp)

    for dx, dy in by_distance(g_places[1]):
        vd = at(dx, dy)
        s = g_places[1].index((dx, dy))
        g_go(1, copy_g.at[held_by(vd)], g_par.at[s], slots + s, (g, vd))
    for dx, dy in by_distance(g_places[0]):
        vd = at(dx, dy)
        s = g_places[0].index((dx, dy))
        g_go(0, copy_g.at[vd], g_own.at[s], s, (g, vd))

    w_waits = {}

    def w_go(src, dst, s, dev, dx):
        cp = remote(src, dst, wdev_send_sem.at[s], wdev_recv_sem.at[s], dev)
        go(cp)
        w_waits.setdefault(dx, []).append(cp)

    w_send = (w_send_own, w_send_par)

    def deal(h):
        home = vp if h else v
        for dx, dy in by_distance(w_places[h]):
            vd = at(dx, dy)
            s = w_places[h].index((dx, dy))
            w_send[h][s] = w_all[h][place_ref[g * members + vd]]
            w_go(w_send[h].at[s], weight.at[home], h * slots + s, (g, vd), dx)
        weight[home] = w_all[h][place_ref[g * members + v]]

    recv = (g_own, g_par)

    def core_swap(h):
        return remote(d_send.at[h], d_recv[h].at[pl.ds(0, NZ)], d_sem.at[0, h], d_sem.at[1, h], core_dev)

    def give_core(h):
        local_g[h].wait()
        for cp in g_waits[h]:
            cp.wait_recv()

        def owner_sum(zz, carry):
            e = 2 * (2 * zz + 1 - c)
            first = recv[h][tab_ref[e, 4 * h]].astype(jnp.float32)
            second = recv[h][tab_ref[e, 4 * h + 1]].astype(jnp.float32)
            d_send[h, zz] = (first + second).astype(jnp.bfloat16)
            return carry

        lax.fori_loop(0, NZ, owner_sum, 0)
        go(core_swap(h))

    def chip_sum(h, zt, j):
        e = 2 * (2 * zt + c) + j
        first = recv[h][tab_ref[e, 4 * h + 2]].astype(jnp.float32)
        second = recv[h][tab_ref[e, 4 * h + 3]].astype(jnp.float32)
        return first + second + d_recv[h][tab_ref[e, 8]].astype(jnp.float32)

    def rs(h, way, step, j):
        return remote(
            r_send.at[h, way, step - 1, j],
            r_recv.at[h, way, step - 1, j],
            rs_send_sem.at[h, way, step - 1, j],
            rs_recv_sem.at[h, way, step - 1, j],
            z_dev[1 - way],
        )

    def rs_step(h, step):
        for j in (0, 1):
            for way in (0, 1):
                length = hops[h][way]
                if step > length:
                    continue
                away = length - step + 1
                zt = zmod(-away if way == 0 else away)
                if step > 1:
                    rs(h, way, step - 1, j).wait_recv()
                total = chip_sum(h, zt, j)
                if step > 1:
                    total = total + r_recv[h, way, step - 2, j].astype(jnp.float32)
                r_send[h, way, step - 1, j] = total.astype(jnp.bfloat16)
                go(rs(h, way, step, j))

    def rs_last(h):
        for j in (0, 1):
            for way in (0, 1):
                if hops[h][way] > 0:
                    rs(h, way, hops[h][way], j).wait_recv()

    def home_sum(h, j):
        total = chip_sum(h, z, j)
        for way in (0, 1):
            if hops[h][way] > 0:
                total = total + r_recv[h, way, hops[h][way] - 1, j].astype(jnp.float32)
        return total

    steps = NZ // 2
    forward(0, 1)
    forward(0, 2)
    pair_copy.wait_recv()
    launch(1, None)
    forward(0, 3)
    forward(1, 1)
    table_copy.wait()
    give_core(1)
    for k in range(4, steps + 1):
        forward(0, k)
    forward(1, 2)
    core_swap(1).wait_recv()
    rs_step(1, 1)
    local_w.wait()
    core_arrived(0)
    deal(0)
    forward(1, 3)
    rs_step(1, 2)
    for k in range(4, steps + 1):
        forward(1, k)
    core_arrived(1)
    deal(1)
    rs_step(1, 3)
    give_core(0)
    core_swap(0).wait_recv()
    rs_step(0, 1)
    for step in range(4, steps + 1):
        rs_step(1, step)
    if steps > 1:
        rs_step(0, 2)
    rs_last(1)
    for j in (0, 1):
        p_send[j] = home_sum(1, j).astype(jnp.bfloat16)
    back = remote(p_send, p_recv, pair_sem.at[2], pair_sem.at[3], up_dev)
    go(back)
    for step in range(3, steps + 1):
        rs_step(0, step)

    kept = lax.broadcasted_iota(jnp.int32, (acts_ref.shape[0], NY * rows), 0) < live_ref[0]
    for i, dx in enumerate(sorted(range(NX), key=lambda d: (min(d, NX - d), d))):
        if i == NX - 1:
            rs_last(0)
            back.wait_recv()
            for j in (0, 1):
                grad_ref[j] = home_sum(0, j) + p_recv[j].astype(jnp.float32)
        for cp in w_waits.get(dx, []):
            cp.wait_recv()
        xs = lax.rem(x - dx + NX, NX)
        part = weight[pl.ds(xs * NY, NY)].reshape(NY * rows, width)
        product = lax.dot_general(
            out_ref[...], part, (((1,), (1,)), ((), ())), preferred_element_type=jnp.float32
        )
        in_parts[xs] = jnp.where(kept, product, jnp.zeros((), jnp.float32)).astype(jnp.bfloat16)
    for xs in range(NX):
        rows_ref[:, xs * NY * rows : (xs + 1) * NY * rows] = in_parts[xs]
    for cp in sends:
        cp.wait_send()


def step(placement, live_rows, acts, grad_out, master):
    rows, width = master.shape[1:]
    slots = NX * SPAN
    lanes = min(128, placement.shape[0])
    owners = 2 * NZ
    steps = max(1, NZ // 2)
    dma = pltpu.SemaphoreType.DMA
    vmem = pl.BlockSpec(memory_space=pltpu.VMEM)
    smem = pl.BlockSpec(memory_space=pltpu.SMEM)
    anywhere = pl.BlockSpec(memory_space=pl.ANY)

    def blocks(*lead):
        return pltpu.VMEM(lead + (rows, width), jnp.bfloat16)

    return pl.pallas_call(
        step_kernel,
        name="step",
        out_shape=(
            jax.ShapeDtypeStruct(acts.shape, jnp.bfloat16),
            jax.ShapeDtypeStruct(master.shape, jnp.float32),
        ),
        in_specs=[smem, vmem, smem, anywhere, anywhere, anywhere],
        out_specs=(vmem, vmem),
        scratch_shapes=[
            pltpu.VMEM((2 * owners, 128), jnp.int32),
            pltpu.SMEM((2 * owners, 128), jnp.int32),
            pltpu.VMEM(acts.shape, acts.dtype),
            pltpu.VMEM(grad_out.shape, grad_out.dtype),
            pltpu.VMEM(master.shape, master.dtype),
            blocks(2),
            blocks(NX * NY),
            blocks(NX * NY),
            pltpu.VMEM((NX, acts.shape[0], NY * rows), jnp.bfloat16),
            blocks(2 * owners),
            blocks(2 * owners),
            blocks(slots),
            blocks(slots),
            blocks(slots + 1),
            blocks(slots + 1),
            blocks(2, NZ),
            blocks(NZ + 1),
            blocks(NZ + 1),
            blocks(2, 2, steps, 2),
            blocks(2, 2, steps, 2),
            blocks(2),
            blocks(2),
            dma((4,)),
            dma((2, 2, steps, 2)),
            dma((2, 2, steps, 2)),
            dma((2, NZ)),
            dma((2, NZ)),
            dma((2 * slots,)),
            dma((2 * slots,)),
            dma((2 * slots,)),
            dma((2 * slots,)),
            dma((2, 2)),
            dma((2, 2, steps, 2)),
            dma((2, 2, steps, 2)),
            dma((7,)),
        ],
        compiler_params=pltpu.CompilerParams(
            collective_id=0, has_side_effects=True, vmem_limit_bytes=60 * 2**20
        ),
    )(placement, placement.reshape(-1, lanes), live_rows, acts, grad_out, master)


def adam_update(master, moment1, moment2, gradient):
    new_moment1 = beta_first * moment1 + (1.0 - beta_first) * gradient
    new_moment2 = beta_second * moment2 + (1.0 - beta_second) * gradient * gradient
    root = jnp.sqrt(new_moment2 * (correct_first**2 / correct_second))
    ascent = new_moment1 / (root + correct_first * epsilon)
    new_master = master - learn_rate * (ascent + decay_rate * master)
    return (new_master, new_moment1, new_moment2)


def on_device(acts, grad_out, live_rows, placement, master, moment1, moment2):
    grad_in, gradient = step(placement, live_rows, acts, grad_out, master)
    new_master, new_moment1, new_moment2 = adam_update(master, moment1, moment2, gradient)
    return (grad_in, new_master, new_moment1, new_moment2)


def solution(mesh):
    in_specs = (
        P(("group", "dev"), None),
        P(("group", "dev"), None),
        P(("group", "dev")),
        P(),
        P("group", "dev", None),
        P("group", "dev", None),
        P("group", "dev", None),
    )
    out_specs = (
        P(("group", "dev"), None),
        P("group", "dev", None),
        P("group", "dev", None),
        P("group", "dev", None),
    )
    return jax.shard_map(
        on_device, mesh=mesh, in_specs=in_specs, out_specs=out_specs, check_vma=False
    )
```
